128 devices in a mesh: dp: 32 (over z, y, core), tensor: 4 (over x).
Axes of the slice: x: 4, y: 4, z: 4, core: 2. Of those that a mesh axis runs over, the one named last changes fastest.
Arguments:
- tokens: bfloat16 [12288, 2880], P('dp', 'tensor'), may hold values from -6 to 6
- out_grad: bfloat16 [12288, 2880], P('dp', 'tensor'), may hold values from -6 to 6
- route_probs: bfloat16 [12288, 4], P('dp'), may hold values from 0.099609375 to 1
- expert_ids: int32 [12288, 4], P('dp'), may hold values from 0 to 127, all different within a row; in each aligned block of 384 rows (0 to 383, 384 to 767, ...) at most 18 rows name the same one
- placement_map: int32 [128], replicated, may hold values from 0 to 127, each once
- w_gate: bfloat16 [32, 2880, 2880], P('dp', None, 'tensor'), may hold values from -0.109375 to 0.109375
- w_up: bfloat16 [32, 2880, 2880], P('dp', None, 'tensor'), may hold values from -0.109375 to 0.109375
- w_down: bfloat16 [32, 2880, 2880], P('dp', 'tensor'), may hold values from -0.109375 to 0.109375
Outputs:
- input_grad: bfloat16 [12288, 2880], P('dp', 'tensor')
- gate_grad: bfloat16 [32, 2880, 2880], P('dp', None, 'tensor')
- up_grad: bfloat16 [32, 2880, 2880], P('dp', None, 'tensor')
- down_grad: bfloat16 [32, 2880, 2880], P('dp', 'tensor')
- prob_grad: bfloat16 [12288, 4], P('dp')
The draws below stay inside these ranges and needn't reach their ends.
Inputs may be any that keep to these rules, and one draw needn't show every extreme that they name: `expert_ids`: each row names 4 different experts. In the rows of one index of dp no expert is named by more than 18 rows, a bound that some block reaches. `placement_map`: A permutation: every value is taken by exactly one expert.
All inputs are finite; a program needn't handle non-finite values.
Results may differ from the reference program's by a relative error of at most 0.011.
Values may be sent and summed in bfloat16 or wider, within the bound.
No kernel may reach another device: no remote copies, remote signals or barrier semaphores. Data moves between devices by JAX's collectives and lax.ppermute only.
A program may use at most 128 MiB of HBM per device.

```python
import math
import jax
import jax.numpy as jnp
import numpy as np
from jax import lax

D = 2880
FF = 2880
TOP = 4
EXP_OWN = 4
EXPERTS = 128
TOK_DEV = 384
TOKENS = 12288
CAP = 18
N_DP = 32
N_TENSOR = 4


def steps_of(rng, dims, split, least, high):
    loudness, own = 1.0, jax.random.fold_in(rng, 6)
    for dim, blocks in split:
        draws = jnp.exp(jax.random.uniform(jax.random.fold_in(own, dim), (blocks,), jnp.float32, least / len(split), high / len(split)))
        loudness = loudness * jnp.repeat(draws, dims[dim] // blocks).reshape([-1 if axis == dim else 1 for axis in range(len(dims))])
    return loudness


def deal_out(own_key, own, number, rows, count, top, limit, slope):
    sequence = jax.random.permutation(own_key, count)
    packed, ordinary = shares(count, rows * top, limit, slope, True), shares(count, rows * top, limit, slope, False)
    places = jnp.arange(count)

    def named(tallies, offset_by):
        used = int((tallies > 0).sum())
        fixed = max(1, used // 4)
        passed = fixed + (places - fixed + offset_by * (used - fixed)) % max(1, count - fixed)
        return jnp.zeros((count,), jnp.int32).at[sequence[jnp.where(places < fixed, places, passed)]].set(jnp.asarray(tallies, jnp.int32))

    tallies = jnp.where(number % 4 == 0, named(packed, number // 4), named(ordinary, number - number // 4 - 1))
    mixed = jax.random.permutation(jax.random.fold_in(own, 3), count)
    donor, receiver = mixed[0:count // 2 * 2:2], mixed[1:count // 2 * 2:2]
    slack = jnp.minimum(tallies[donor] - 1, limit - tallies[receiver]) // 2
    slack = jnp.where((donor == sequence[0]) | (receiver == sequence[0]) | (tallies[receiver] == 0), 0, jnp.maximum(slack, 0))
    passed = jax.random.randint(jax.random.fold_in(own, 4), (count // 2,), 0, 1 << 20) % (slack + 1)
    tallies = tallies.at[donor].add(-passed).at[receiver].add(passed)
    members = jnp.searchsorted(jnp.cumsum(tallies), jnp.arange(rows * top), side="right").astype(jnp.int32)
    table = members.reshape(top, rows).T
    table = table[jax.random.permutation(jax.random.fold_in(own, 1), rows)]
    offset_by = jax.random.randint(jax.random.fold_in(own, 2), (rows, 1), 0, top)
    return jnp.take_along_axis(table, (jnp.arange(top)[None, :] + offset_by) % top, axis=1)


def shares(amount, total, reach, slope, full):
    loads = [(1 << 20) // math.isqrt(rank ** slope) + 1 for rank in range(1, amount + 1)]
    largest = reach if full else min(reach, max(-(-total // amount), total * loads[0] // sum(loads)))
    least = 1 if total - largest >= amount - 1 else 0
    counts, surplus = [largest] + [least] * (amount - 1), total - largest - least * (amount - 1)
    while surplus > 0:
        candidates = [i for i in range(1, amount) if counts[i] < largest] or [i for i in range(1, amount) if counts[i] < reach]
        mass, left = sum([loads[i] for i in candidates]), surplus
        for i in candidates:
            extra = min(reach - counts[i], max(1, left * loads[i] // mass), surplus)
            counts[i] = counts[i] + extra
            surplus = surplus - extra
    return np.array(counts)


def scatter_about(own_key, extent, deviation, most, shards=(), kind=jnp.bfloat16):
    array = deviation * jax.random.normal(own_key, extent, jnp.float32)
    if shards:
        array = array * steps_of(own_key, extent, shards, -0.22, 0.18)
    return jnp.clip(array, -most, most).astype(kind)


def setup_inputs(seed: int = 0) -> dict:
    splits = jax.random.split(jax.random.key(seed), 9)
    tokens = scatter_about(splits[0], (TOKENS, D), 1.0, 6.0, ((0, 32), (1, 4)))
    out_grad = scatter_about(splits[1], (TOKENS, D), 1.0, 6.0, ((0, 32), (1, 4)))
    route_probs = jnp.clip(0.099609375 + 0.9003906 * jax.random.uniform(splits[2], (TOKENS, TOP), jnp.float32) ** steps_of(splits[2], (TOKENS, TOP), ((0, 32),), -0.2, 0.2), 0.099609375, 1.0).astype(jnp.bfloat16)
    expert_ids_keys = jax.random.split(jax.random.fold_in(splits[3], 1), TOKENS // TOK_DEV)
    expert_ids_turns = jax.random.permutation(jax.random.fold_in(splits[3], 3), TOKENS // TOK_DEV)
    expert_ids = jax.vmap(lambda own, number: deal_out(jax.random.fold_in(splits[3], 2), own, number, TOK_DEV, EXPERTS, TOP, CAP, 2))(expert_ids_keys, expert_ids_turns).reshape((TOKENS, TOP))
    placement_map = jax.random.permutation(splits[4], EXPERTS).astype(jnp.int32)
    w_gate = scatter_about(splits[5], (N_DP, D, FF), D ** -0.5, 0.109375, ((0, 32), (2, 4)))
    w_up = scatter_about(splits[6], (N_DP, D, FF), D ** -0.5, 0.109375, ((0, 32), (2, 4)))
    w_down = scatter_about(splits[7], (N_DP, FF, D), FF ** -0.5, 0.109375, ((0, 32), (1, 4)))
    return {"tokens": tokens, "out_grad": out_grad, "route_probs": route_probs, "expert_ids": expert_ids, "placement_map": placement_map, "w_gate": w_gate, "w_up": w_up, "w_down": w_down}


SWISH_SLOPE = 1.702


def wave_layout(expert_ids, placement_map):
    code_value = placement_map[expert_ids].reshape(N_DP, TOK_DEV * TOP)
    in_wave = code_value % EXP_OWN == 0
    owner_of = code_value // EXP_OWN
    owner_range = jnp.arange(N_DP, dtype=jnp.int32)
    chosen = ((owner_of[:, :, None] == owner_range[None, None, :]) & in_wave[:, :, None]).astype(jnp.int32)
    before = jnp.cumsum(chosen, axis=1) - chosen
    slot_index = jnp.sum(before * chosen, axis=2).astype(jnp.int32)
    position = owner_range[:, None] * CAP + slot_index
    return in_wave, owner_of, position


def reference(tokens, out_grad, route_probs, expert_ids, placement_map, w_gate, w_up, w_down):
    in_wave, owner_of, position = wave_layout(expert_ids, placement_map)
    route_ids = jnp.arange(TOKENS * TOP, dtype=jnp.int32).reshape(N_DP, TOK_DEV * TOP)
    owner_row = jnp.where(in_wave, owner_of, N_DP).astype(jnp.int32)
    slot_route = jnp.full((N_DP, N_DP * CAP), -1, jnp.int32).at[owner_row, position].set(route_ids, mode="drop")
    flat_probs = route_probs.reshape(-1)
    zero_half = jnp.zeros((), jnp.bfloat16)
    block_width = FF // N_TENSOR

    def expert_backward(operands):
        gate_w, up_w, down_w, routes = operands
        row_valid = routes >= 0
        safe_route = jnp.where(row_valid, routes, 0).astype(jnp.int32)
        token_index = (safe_route // TOP).astype(jnp.int32)
        rows_x = jnp.where(row_valid[:, None], tokens[token_index], zero_half)
        rows_d = jnp.where(row_valid[:, None], out_grad[token_index], zero_half)
        prob_column = jnp.where(row_valid, flat_probs[safe_route], zero_half).astype(jnp.float32)[:, None]
        gate_pre = jnp.dot(rows_x, gate_w, preferred_element_type=jnp.float32)
        up_pre = jnp.dot(rows_x, up_w, preferred_element_type=jnp.float32)
        sig_gate = jax.nn.sigmoid(SWISH_SLOPE * gate_pre)
        active = (gate_pre * sig_gate * (up_pre + 1.0)).astype(jnp.bfloat16)
        down_back = jnp.dot(rows_d, down_w.T, preferred_element_type=jnp.float32)
        prob_sum = jnp.sum(active.astype(jnp.float32) * down_back, axis=1)
        delta_act = prob_column * down_back
        grad_gate_pre = (delta_act * (up_pre + 1.0) * (sig_gate + SWISH_SLOPE * gate_pre * sig_gate * (1.0 - sig_gate))).astype(jnp.bfloat16)
        grad_up_pre = (delta_act * gate_pre * sig_gate).astype(jnp.bfloat16)
        scaled_grad = (prob_column * rows_d.astype(jnp.float32)).astype(jnp.bfloat16)
        down_grad = jnp.dot(active.T, scaled_grad, preferred_element_type=jnp.float32).astype(jnp.bfloat16)
        gate_grad = jnp.dot(rows_x.T, grad_gate_pre, preferred_element_type=jnp.float32).astype(jnp.bfloat16)
        up_grad = jnp.dot(rows_x.T, grad_up_pre, preferred_element_type=jnp.float32).astype(jnp.bfloat16)
        input_total = jnp.zeros((routes.shape[0], D), jnp.float32)
        for block in range(N_TENSOR):
            lower = block * block_width
            upper = lower + block_width
            partial_rows = (jnp.dot(grad_gate_pre[:, lower:upper], gate_w[:, lower:upper].T, preferred_element_type=jnp.float32)
                            + jnp.dot(grad_up_pre[:, lower:upper], up_w[:, lower:upper].T, preferred_element_type=jnp.float32))
            input_total = input_total + partial_rows.astype(jnp.bfloat16).astype(jnp.float32)
        input_rows = input_total.astype(jnp.bfloat16)
        return gate_grad, up_grad, down_grad, input_rows, prob_sum.astype(jnp.bfloat16)

    gate_grad, up_grad, down_grad, back_rows, back_prob = lax.map(expert_backward, (w_gate, w_up, w_down, slot_route))
    flat_index = (jnp.where(in_wave, owner_of, 0) * (N_DP * CAP) + jnp.where(in_wave, position, 0)).reshape(-1).astype(jnp.int32)
    wave_flat = in_wave.reshape(-1)
    route_rows = jnp.where(wave_flat[:, None], back_rows.reshape(N_DP * N_DP * CAP, D)[flat_index], zero_half)
    input_grad = jnp.sum(route_rows.reshape(TOKENS, TOP, D).astype(jnp.float32), axis=1).astype(jnp.bfloat16)
    prob_grad = jnp.where(wave_flat, back_prob.reshape(-1)[flat_index], zero_half).reshape(TOKENS, TOP)
    return input_grad, gate_grad, up_grad, down_grad, prob_grad
```

```python
import functools

import jax
import jax.numpy as jnp
from jax import lax
from jax.experimental import pallas as pl
from jax.experimental.pallas import tpu as pltpu
from jax.sharding import PartitionSpec as P


SWISH_SLOPE = 1.702
EXP_OWN = 4
OWNERS = 32
CAP = 18
MAIN = 16
ROWS = OWNERS * CAP
MROWS = OWNERS * MAIN
TOK = 384
TOP = 4
WID = 720
PAD = 768
FEAT = 2880
FPAD = 2944
SIDES = 4
PROB = 720

BF = jnp.bfloat16
F32 = jnp.float32
NT = (((1,), (1,)), ((), ()))
TN = (((0,), (0,)), ((), ()))
NN = (((1,), (0,)), ((), ()))


def dot(a, b, dims):
    return lax.dot_general(a, b, dims, preferred_element_type=F32)


def call(body, out_shape, **kw):
    params = pltpu.CompilerParams(vmem_limit_bytes=kw.pop("vmem", 56 << 20), **({"dimension_semantics": ("arbitrary",)} if "grid" in kw else {}))
    flops = kw.pop("flops", 0)
    nbytes = kw.pop("nbytes", 4 << 20)
    return pl.pallas_call(
        body,
        out_shape=out_shape,
        compiler_params=params,
        cost_estimate=pl.CostEstimate(flops=flops, bytes_accessed=nbytes, transcendentals=0),
        **kw,
    )


def struct(shape, dtype=BF):
    return jax.ShapeDtypeStruct(shape, dtype)


def vm():
    return pl.BlockSpec(memory_space=pltpu.VMEM)


def sm():
    return pl.BlockSpec(memory_space=pltpu.SMEM)


def iota(shape, dim):
    return lax.broadcasted_iota(jnp.int32, shape, dim)


def swap_matrix():
    r, q = iota((128, 128), 0), iota((128, 128), 1)
    return (((r >> 4) == ((q >> 1) & 7)) & ((q >> 4) == ((r >> 1) & 7)) & ((r & 1) == (q & 1))).astype(BF)


def tiles_of(width):
    return width // 128


def block_rows(width):
    t = tiles_of(width)
    return MAIN * t + 16 * ((t + 7) // 8)


def pack_rest(rest, out_ref, width):
    t = tiles_of(width)
    swap = swap_matrix()
    for a in range((t + 7) // 8):
        for i in range(OWNERS // 8):
            parts = [
                rest[16 * i : 16 * i + 16, 128 * j : 128 * j + 128] if j < t else jnp.zeros((16, 128), BF)
                for j in range(8 * a, 8 * a + 8)
            ]
            turned = dot(swap, jnp.concatenate(parts, axis=0), NN).astype(BF)
            out_ref[8 * i : 8 * i + 8, MAIN * t + 16 * a : MAIN * t + 16 * a + 16, :] = turned.reshape(8, 16, 128)


def unpack(ref, width, store, first=0):
    t = tiles_of(width)
    peers = ref.shape[0]
    for j in range(t):
        store(MAIN * first, 128 * j, ref[:, MAIN * j : MAIN * j + MAIN, :].reshape(MAIN * peers, 128))
    swap = swap_matrix()
    for a in range((t + 7) // 8):
        for i in range(peers // 8):
            block = ref[8 * i : 8 * i + 8, MAIN * t + 16 * a : MAIN * t + 16 * a + 16, :].reshape(128, 128)
            turned = dot(swap, block, NN).astype(BF)
            for b in range(8):
                j = 8 * a + b
                if j < t:
                    store(MROWS + 2 * first + 16 * i, 128 * j, turned[16 * b : 16 * b + 16])


def row_owner(shape, dim):
    r = iota(shape, dim)
    return jnp.where(r < MROWS, r >> 4, (r - MROWS) >> 1)


def row_slot(shape, dim):
    r = iota(shape, dim)
    return jnp.where(r < MROWS, r & 15, MAIN + (r & 1))


def hits_of(ids_ref, map_ref):
    experts = map_ref.shape[1]
    eq = map_ref[...] == EXP_OWN * iota((OWNERS, experts), 0)
    held = jnp.sum(jnp.where(eq, iota((OWNERS, experts), 1), 0), axis=1, keepdims=True)
    return [ids_ref[k : k + 1, :] == held for k in range(TOP)]


def dispatch_x_body(ids_ref, prob_ref, map_ref, tok_ref, send_ref, pick_ref, tokp, rest):
    hits = hits_of(ids_ref, map_ref)
    probs = prob_ref[...].astype(F32)
    named = hits[0] | hits[1] | hits[2] | hits[3]
    p_on = jnp.zeros((OWNERS, TOK), F32)
    for k in range(TOP):
        p_on = jnp.where(hits[k], probs[k : k + 1, :], p_on)
    upper = (iota((TOK, TOK), 0) < iota((TOK, TOK), 1)).astype(F32).astype(BF)
    rank = dot(named.astype(F32).astype(BF), upper, NN)
    key = jnp.where(named, rank, -1.0).astype(BF)
    spread = (row_owner((ROWS, OWNERS), 0) == iota((ROWS, OWNERS), 1)).astype(F32).astype(BF)
    pick = dot(spread, key, NN) == row_slot((ROWS, TOK), 0).astype(F32)
    p_col = jnp.sum(jnp.where(pick, dot(spread, p_on.astype(BF), NN), 0.0), axis=1, keepdims=True)
    pick = pick.astype(F32).astype(BF)
    pick_ref[...] = pick
    tokp[0:WID, :] = tok_ref[...]
    tokp[WID:PAD, :] = jnp.zeros((PAD - WID, TOK), BF)
    for q in range(3):
        val = dot(pick, tokp[256 * q : 256 * q + 256, :], NT)
        if q == 2:
            val = jnp.where(iota((ROWS, 256), 1) == PROB - 512, p_col, val)
        val = val.astype(BF)
        for j in (2 * q, 2 * q + 1):
            tile = val[:, 128 * (j - 2 * q) : 128 * (j - 2 * q) + 128]
            send_ref[:, MAIN * j : MAIN * j + MAIN, :] = tile[:MROWS].reshape(OWNERS, MAIN, 128)
            rest[:, 128 * j : 128 * j + 128] = tile[MROWS:]
    pack_rest(rest, send_ref, PAD)


def dispatch_d_body(t_ref, pick_ref, own_ref, below_ref, above_ref, far_a_ref, far_b_ref, send_ref, full, rest):
    t = t_ref[0]

    def put(side, ref, off, rows):
        j = lax.rem(t + side, SIDES)
        full[pl.ds(pl.multiple_of(WID * j + off, 16), rows), :] = ref[...]

    put(0, own_ref, 0, WID)
    put(3, below_ref, 0, WID)
    put(1, above_ref, 0, WID)
    put(2, far_a_ref, 0, 368)
    put(2, far_b_ref, 368, WID - 368)
    full[FEAT:3072, :] = jnp.zeros((3072 - FEAT, TOK), BF)
    pick = pick_ref[...]
    for q in range(12):
        val = dot(pick, full[256 * q : 256 * q + 256, :], NT).astype(BF)
        for j in (2 * q, 2 * q + 1):
            if j < tiles_of(FPAD):
                tile = val[:, 128 * (j - 2 * q) : 128 * (j - 2 * q) + 128]
                send_ref[:, MAIN * j : MAIN * j + MAIN, :] = tile[:MROWS].reshape(OWNERS, MAIN, 128)
                rest[:, 128 * j : 128 * j + 128] = tile[MROWS:]
    pack_rest(rest, send_ref, FPAD)


def turn_body(t_ref, w_ref, out_ref):
    t = t_ref[0]
    for j in range(SIDES):
        k = lax.rem(j - t + SIDES, SIDES)
        piece = w_ref[:, WID * j : WID * j + WID]
        full = jnp.concatenate([piece, jnp.zeros((piece.shape[0], PAD - WID), BF)], axis=1)
        out_ref[pl.ds(k, 1), :, :] = full[None]


def gate_up_body(own_ref, below_ref, above_ref, far_a_ref, far_b_ref, wg_ref, wu_ref, gate_ref, up_ref, x_ref, p_ref):
    @pl.when(pl.program_id(0) == 0)
    def _():
        def keep(side):
            def store(row, lane, value):
                x_ref[side, row : row + value.shape[0], lane : lane + 128] = value

            return store

        unpack(own_ref, PAD, keep(0))
        unpack(above_ref, PAD, keep(1))
        unpack(below_ref, PAD, keep(3))
        unpack(far_a_ref, PAD, keep(2), 0)
        unpack(far_b_ref, PAD, keep(2), OWNERS // 2)
        tile = x_ref[0, :, 640:768].astype(F32)
        p_ref[...] = jnp.sum(jnp.where(iota((ROWS, 128), 1) == PROB - 640, tile, 0.0), axis=1, keepdims=True)

    for w_ref, out_ref in ((wg_ref, gate_ref), (wu_ref, up_ref)):
        total = dot(x_ref[0], w_ref[0], NT)
        for side in range(1, SIDES):
            total = total + dot(x_ref[side], w_ref[side], NT)
        out_ref[...] = total


def back_body(got_ref, wd_ref, gate_ref, up_ref, p_ref, d_ref, act_ref, gg_ref, gu_ref, prob_ref):
    step = pl.program_id(0)

    @pl.when(step == 0)
    def _():
        def store(row, lane, value):
            width = min(128, FEAT - lane)
            d_ref[row : row + value.shape[0], lane : lane + width] = value[:, :width]

        unpack(got_ref, FPAD, store)
        prob_ref[...] = jnp.zeros_like(prob_ref)

    down_back = dot(d_ref[...], wd_ref[...], NT)
    gate = gate_ref[...]
    up1 = up_ref[...] + 1.0
    sig = 1.0 / (1.0 + jnp.exp(-SWISH_SLOPE * gate))
    act = (gate * sig * up1).astype(BF)
    act_ref[...] = act
    delta = p_ref[...] * down_back
    gg_ref[...] = (delta * up1 * (sig + SWISH_SLOPE * gate * sig * (1.0 - sig))).astype(BF)
    gu_ref[...] = (delta * gate * sig).astype(BF)
    inside = iota(act.shape, 1) + 256 * step < WID
    part = jnp.sum(jnp.where(inside, act.astype(F32) * down_back, 0.0), axis=1, keepdims=True)
    prob_ref[...] += jnp.where(iota((ROWS, 128), 1) == PROB - 640, part, 0.0)


def split_prob(tile):
    lane = iota(tile.shape, 1)
    total = jnp.sum(jnp.where(lane == PROB - 640, tile, 0.0), axis=1, keepdims=True)
    high = total.astype(BF).astype(F32)
    return jnp.where(lane == PROB - 640, high, jnp.where(lane == PROB - 639, total - high, tile))


def join_prob(tile):
    lane = iota(tile.shape, 1)
    total = jnp.sum(jnp.where((lane == PROB - 640) | (lane == PROB - 639), tile, 0.0), axis=1, keepdims=True)
    return jnp.where(lane == PROB - 640, total, jnp.where(lane == PROB - 639, 0.0, tile))


def far_dx_body(gg_ref, gu_ref, wg_ref, wu_ref, prob_ref, a_ref, b_ref):
    half = ROWS // 2
    val = dot(gg_ref[...], wg_ref[0], NN) + dot(gu_ref[...], wu_ref[0], NN)
    tile = split_prob(val[:, 640:768] + prob_ref[...]).astype(BF)
    val = val[:, :640].astype(BF)
    a_ref[:, 0:640] = val[:half]
    b_ref[:, 0:640] = val[half:]
    a_ref[:, 640:768] = tile[:half]
    b_ref[:, 640:768] = tile[half:]


def near_dx_body(gg_ref, gu_ref, wg_ref, wu_ref, prob_ref, out_ref):
    val = dot(gg_ref[...], wg_ref[0], NN) + dot(gu_ref[...], wu_ref[0], NN)
    out_ref[0, :, 0:640] = val[:, :640]
    out_ref[0, :, 640:768] = val[:, 640:768] + prob_ref[...]


def relay_body(dx_ref, a_ref, b_ref, above_ref, below_ref):
    half = ROWS // 2
    for ref, out, add, lo in ((dx_ref.at[0], above_ref, a_ref, 0), (dx_ref.at[1], below_ref, b_ref, half)):
        other = half - lo
        out[other : other + half, 0:640] = ref[other : other + half, 0:640].astype(BF)
        out[other : other + half, 640:768] = split_prob(ref[other : other + half, 640:768]).astype(BF)
        out[lo : lo + half, 0:640] = (ref[lo : lo + half, 0:640] + add[:, 0:640].astype(F32)).astype(BF)
        tile = ref[lo : lo + half, 640:768] + join_prob(add[:, 640:768].astype(F32))
        out[lo : lo + half, 640:768] = split_prob(tile).astype(BF)


def sum_body(own_ref, below_ref, above_ref, send_ref, rest):
    for j in range(tiles_of(PAD)):
        cols = slice(128 * j, 128 * j + 128)
        tile = own_ref[0, :, cols] + below_ref[:, cols].astype(F32) + above_ref[:, cols].astype(F32)
        if j == 5:
            tile = join_prob(tile)
        tile = tile.astype(BF)
        send_ref[:, MAIN * j : MAIN * j + MAIN, :] = tile[:MROWS].reshape(OWNERS, MAIN, 128)
        rest[:, cols] = tile[MROWS:]
    pack_rest(rest, send_ref, PAD)


def combine_body(back_ref, pick_ref, ids_ref, map_ref, dx_ref, dp_ref, rows):
    def store(row, lane, value):
        rows[row : row + value.shape[0], lane : lane + 128] = value

    unpack(back_ref, PAD, store)
    pick = pick_ref[...]
    dx_ref[...] = dot(rows[...], pick, TN)[:WID].astype(BF)
    tile = rows[:, 640:768].astype(F32)
    p_col = jnp.sum(jnp.where(iota((ROWS, 128), 1) == PROB - 640, tile, 0.0), axis=1, keepdims=True)
    spread = (row_owner((OWNERS, ROWS), 1) == iota((OWNERS, ROWS), 0)).astype(F32).astype(BF)
    per_owner = dot(spread, (pick.astype(F32) * p_col).astype(BF), NN)
    hits = hits_of(ids_ref, map_ref)
    for k in range(TOP):
        dp_ref[k : k + 1, :] = jnp.sum(jnp.where(hits[k], per_owner, 0.0), axis=0, keepdims=True).astype(BF)


def grad_pair_body(t_ref, x_ref, gg_ref, gu_ref, gate_ref, up_ref):
    t = t_ref[0]
    for j in range(SIDES):
        k = lax.rem(j - t + SIDES, SIDES)
        x = x_ref[pl.ds(k, 1)][0]
        for src, out in ((gg_ref, gate_ref), (gu_ref, up_ref)):
            out[:, WID * j : WID * j + WID] = dot(src[...], x, TN).astype(BF)[:, :WID]


def down_body(d_ref, act_ref, p_ref, out_ref, scaled):
    @pl.when(pl.program_id(0) == 0)
    def _():
        scaled[...] = (d_ref[...].astype(F32) * p_ref[...]).astype(BF)

    out_ref[...] = dot(act_ref[...], scaled[...], TN).astype(BF)


def turn(w, t):
    return call(
        turn_body,
        struct((SIDES, WID, PAD)),
        grid=(3,),
        in_specs=[sm(), pl.BlockSpec((240, FEAT), lambda i: (i, 0))],
        out_specs=pl.BlockSpec((SIDES, 240, PAD), lambda i: (0, i, 0)),
    )(t, w)


def whole(shape):
    return pl.BlockSpec(shape, lambda i: (0,) * len(shape))


def shards(tokens, out_grad, route_probs, expert_ids, placement_map, w_gate, w_up, w_down):
    above = [((i + 1) % SIDES, i) for i in range(SIDES)]
    below = [((i - 1) % SIDES, i) for i in range(SIDES)]
    t = lax.axis_index("tensor").astype(jnp.int32).reshape(1)
    tok_t, d_t, ids_t, prob_t = tokens.T, out_grad.T, expert_ids.T, route_probs.T
    pmap = placement_map.reshape(1, -1)
    wg_t, wu_t, wd = w_gate[0].T, w_up[0].T, w_down[0]
    d_above = lax.ppermute(d_t, "tensor", above)
    d_below = lax.ppermute(d_t, "tensor", below)
    bx = block_rows(PAD)
    bd = block_rows(FPAD)
    send_x, pick = call(
        dispatch_x_body,
        (struct((OWNERS, bx, 128)), struct((ROWS, TOK))),
        in_specs=[vm()] * 4,
        out_specs=(vm(), vm()),
        scratch_shapes=[pltpu.VMEM((PAD, TOK), BF), pltpu.VMEM((ROWS - MROWS, PAD), BF)],
        flops=10**9,
    )(ids_t, prob_t, pmap, tok_t)
    got_x = lax.all_to_all(send_x, "dp", 0, 0, tiled=True)
    d_far_a = lax.ppermute(d_below[:368], "tensor", below)
    d_far_b = lax.ppermute(d_above[368:], "tensor", above)
    wg, wu = turn(wg_t, t), turn(wu_t, t)
    x_above = lax.ppermute(got_x, "tensor", above)
    x_below = lax.ppermute(got_x, "tensor", below)
    send_d = call(
        dispatch_d_body,
        struct((OWNERS, bd, 128)),
        in_specs=[sm()] + [vm()] * 6,
        out_specs=vm(),
        scratch_shapes=[pltpu.VMEM((3072, TOK), BF), pltpu.VMEM((ROWS - MROWS, FPAD), BF)],
        flops=2 * 10**9,
    )(t, pick, d_t, d_below, d_above, d_far_a, d_far_b)
    got_d = lax.all_to_all(send_d, "dp", 0, 0, tiled=True)
    x_far_a = lax.ppermute(x_below[: OWNERS // 2], "tensor", below)
    x_far_b = lax.ppermute(x_above[OWNERS // 2 :], "tensor", above)
    act_spec = pl.BlockSpec((ROWS, 256), lambda i: (0, i))
    row_spec = pl.BlockSpec((256, FEAT), lambda i: (i, 0))
    w_spec = pl.BlockSpec((SIDES, 256, PAD), lambda i: (0, i, 0))
    gate, up, x_rel, p_col = call(
        gate_up_body,
        (struct((ROWS, WID), F32), struct((ROWS, WID), F32), struct((SIDES, ROWS, PAD)), struct((ROWS, 1), F32)),
        grid=(3,),
        in_specs=[whole((OWNERS, bx, 128))] * 3 + [whole((OWNERS // 2, bx, 128))] * 2 + [w_spec] * 2,
        out_specs=(act_spec, act_spec, whole((SIDES, ROWS, PAD)), whole((ROWS, 1))),
        flops=5 * 10**9,
    )(got_x, x_below, x_above, x_far_a, x_far_b, wg, wu)
    d_rows, act, gg, gu, prob = call(
        back_body,
        (struct((ROWS, FEAT)), struct((ROWS, WID)), struct((ROWS, WID)), struct((ROWS, WID)), struct((ROWS, 128), F32)),
        grid=(3,),
        in_specs=[whole((OWNERS, bd, 128)), row_spec, act_spec, act_spec, whole((ROWS, 1))],
        out_specs=(whole((ROWS, FEAT)), act_spec, act_spec, act_spec, whole((ROWS, 128))),
        flops=3 * 10**9,
    )(got_d, wd, gate, up, p_col)
    half = struct((ROWS // 2, PAD))
    dx_ins = lambda which: [
        whole((ROWS, WID)),
        whole((ROWS, WID)),
        pl.BlockSpec((1, WID, PAD), lambda i: (which(i), 0, 0)),
        pl.BlockSpec((1, WID, PAD), lambda i: (which(i), 0, 0)),
        whole((ROWS, 128)),
    ]
    part_a, part_b = call(
        far_dx_body,
        (half, half),
        grid=(1,),
        in_specs=dx_ins(lambda i: 2),
        out_specs=(whole((ROWS // 2, PAD)), whole((ROWS // 2, PAD))),
        flops=12 * 10**8,
    )(gg, gu, wg, wu, prob)
    came_a = lax.ppermute(part_a, "tensor", below)
    came_b = lax.ppermute(part_b, "tensor", above)
    near = call(
        near_dx_body,
        struct((3, ROWS, PAD), F32),
        grid=(3,),
        in_specs=dx_ins(lambda i: jnp.where(i == 0, 1, jnp.where(i == 1, 3, 0))),
        out_specs=pl.BlockSpec((1, ROWS, PAD), lambda i: (i, 0, 0)),
        flops=36 * 10**8,
    )(gg, gu, wg, wu, prob)
    to_above, to_below = call(
        relay_body,
        (struct((ROWS, PAD)), struct((ROWS, PAD))),
        grid=(1,),
        in_specs=[pl.BlockSpec((2, ROWS, PAD), lambda i: (0, 0, 0)), whole((ROWS // 2, PAD)), whole((ROWS // 2, PAD))],
        out_specs=(whole((ROWS, PAD)), whole((ROWS, PAD))),
    )(near, came_a, came_b)
    from_below = lax.ppermute(to_above, "tensor", below)
    from_above = lax.ppermute(to_below, "tensor", above)
    gate_grad, up_grad = call(
        grad_pair_body,
        (struct((WID, FEAT)), struct((WID, FEAT))),
        grid=(3,),
        in_specs=[sm(), whole((SIDES, ROWS, PAD)), act_spec, act_spec],
        out_specs=(row_spec, row_spec),
        flops=5 * 10**9,
    )(t, x_rel, gg, gu)
    down_grad = call(
        down_body,
        struct((WID, FEAT)),
        grid=(3,),
        in_specs=[whole((ROWS, FEAT)), act_spec, whole((ROWS, 1))],
        out_specs=row_spec,
        scratch_shapes=[pltpu.VMEM((ROWS, FEAT), BF)],
        flops=3 * 10**9,
    )(d_rows, act, p_col)
    send_back = call(
        sum_body,
        struct((OWNERS, bx, 128)),
        grid=(1,),
        in_specs=[pl.BlockSpec((1, ROWS, PAD), lambda i: (2, 0, 0)), whole((ROWS, PAD)), whole((ROWS, PAD))],
        out_specs=whole((OWNERS, bx, 128)),
        scratch_shapes=[pltpu.VMEM((ROWS - MROWS, PAD), BF)],
    )(near, from_below, from_above)
    back = lax.all_to_all(send_back, "dp", 0, 0, tiled=True)
    dx_t, dp_t = call(
        combine_body,
        (struct((WID, TOK)), struct((TOP, TOK))),
        in_specs=[vm()] * 4,
        out_specs=(vm(), vm()),
        scratch_shapes=[pltpu.VMEM((ROWS, PAD), BF)],
        flops=10**9,
    )(back, pick, ids_t, pmap)
    return dx_t.T, gate_grad.T[None], up_grad.T[None], down_grad[None], dp_t.T


def solution(mesh):
    in_specs = (
        P("dp", "tensor"),
        P("dp", "tensor"),
        P("dp", None),
        P("dp", None),
        P(),
        P("dp", None, "tensor"),
        P("dp", None, "tensor"),
        P("dp", "tensor", None),
    )
    out_specs = (
        P("dp", "tensor"),
        P("dp", None, "tensor"),
        P("dp", None, "tensor"),
        P("dp", "tensor", None),
        P("dp", None),
    )
    return jax.shard_map(shards, mesh=mesh, in_specs=in_specs, out_specs=out_specs, check_vma=False)
```

```python
import jax
import jax.numpy as jnp
from jax import lax
from jax.experimental import pallas as pl
from jax.experimental.pallas import tpu as pltpu
from jax.sharding import PartitionSpec as P


SWISH_SLOPE = 1.702
EXP_OWN = 4
OWNERS = 32
CAP = 18
MAIN = 16
ROWS = OWNERS * CAP
MROWS = OWNERS * MAIN
TOK = 384
TOP = 4
WID = 720
PAD = 768
FEAT = 2880
FPAD = 2944
SIDES = 4
GATE_VMEM = 58
BACK_VMEM = 55
PROB = 720

BF = jnp.bfloat16
F32 = jnp.float32
NT = (((1,), (1,)), ((), ()))
TN = (((0,), (0,)), ((), ()))
NN = (((1,), (0,)), ((), ()))


def dot(a, b, dims):
    return lax.dot_general(a, b, dims, preferred_element_type=F32)


def call(body, out_shape, **kw):
    params = pltpu.CompilerParams(vmem_limit_bytes=kw.pop("vmem", 8) << 20, **({"dimension_semantics": ("arbitrary",)} if "grid" in kw else {}))
    flops = kw.pop("flops", 0)
    nbytes = kw.pop("nbytes", 4 << 20)
    return pl.pallas_call(
        body,
        out_shape=out_shape,
        compiler_params=params,
        cost_estimate=pl.CostEstimate(flops=flops, bytes_accessed=nbytes, transcendentals=0),
        **kw,
    )


def struct(shape, dtype=BF):
    return jax.ShapeDtypeStruct(shape, dtype)


def vm():
    return pl.BlockSpec(memory_space=pltpu.VMEM)


def sm():
    return pl.BlockSpec(memory_space=pltpu.SMEM)


def iota(shape, dim):
    return lax.broadcasted_iota(jnp.int32, shape, dim)


def swap_matrix():
    r, q = iota((128, 128), 0), iota((128, 128), 1)
    return (((r >> 4) == ((q >> 1) & 7)) & ((q >> 4) == ((r >> 1) & 7)) & ((r & 1) == (q & 1))).astype(BF)


def tiles_of(width):
    return width // 128


def block_rows(width):
    t = tiles_of(width)
    return MAIN * t + 16 * ((t + 7) // 8)


def pack_rest(rest, out_ref, width):
    t = tiles_of(width)
    swap = swap_matrix()
    for a in range((t + 7) // 8):
        for i in range(OWNERS // 8):
            parts = [
                rest[16 * i : 16 * i + 16, 128 * j : 128 * j + 128] if j < t else jnp.zeros((16, 128), BF)
                for j in range(8 * a, 8 * a + 8)
            ]
            turned = dot(swap, jnp.concatenate(parts, axis=0), NN).astype(BF)
            out_ref[8 * i : 8 * i + 8, MAIN * t + 16 * a : MAIN * t + 16 * a + 16, :] = turned.reshape(8, 16, 128)


def unpack(ref, width, store, first=0):
    t = tiles_of(width)
    peers = ref.shape[0]
    for j in range(t):
        store(MAIN * first, 128 * j, ref[:, MAIN * j : MAIN * j + MAIN, :].reshape(MAIN * peers, 128))
    swap = swap_matrix()
    for a in range((t + 7) // 8):
        for i in range(peers // 8):
            block = ref[8 * i : 8 * i + 8, MAIN * t + 16 * a : MAIN * t + 16 * a + 16, :].reshape(128, 128)
            turned = dot(swap, block, NN).astype(BF)
            for b in range(8):
                j = 8 * a + b
                if j < t:
                    store(MROWS + 2 * first + 16 * i, 128 * j, turned[16 * b : 16 * b + 16])


def row_owner(shape, dim):
    r = iota(shape, dim)
    return jnp.where(r < MROWS, r >> 4, (r - MROWS) >> 1)


def row_slot(shape, dim):
    r = iota(shape, dim)
    return jnp.where(r < MROWS, r & 15, MAIN + (r & 1))


def hits_of(ids_ref, map_ref):
    experts = map_ref.shape[1]
    eq = map_ref[...] == EXP_OWN * iota((OWNERS, experts), 0)
    held = jnp.sum(jnp.where(eq, iota((OWNERS, experts), 1), 0), axis=1, keepdims=True)
    return [ids_ref[k : k + 1, :] == held for k in range(TOP)]


def dispatch_x_body(ids_ref, prob_ref, map_ref, tok_ref, send_ref, pick_ref, tokp, rest):
    hits = hits_of(ids_ref, map_ref)
    probs = prob_ref[...].astype(F32)
    named = hits[0] | hits[1] | hits[2] | hits[3]
    p_on = jnp.zeros((OWNERS, TOK), F32)
    for k in range(TOP):
        p_on = jnp.where(hits[k], probs[k : k + 1, :], p_on)
    upper = (iota((TOK, TOK), 0) < iota((TOK, TOK), 1)).astype(F32).astype(BF)
    rank = dot(named.astype(F32).astype(BF), upper, NN)
    key = jnp.where(named, rank, -1.0).astype(BF)
    spread = (row_owner((ROWS, OWNERS), 0) == iota((ROWS, OWNERS), 1)).astype(F32).astype(BF)
    pick = dot(spread, key, NN) == row_slot((ROWS, TOK), 0).astype(F32)
    p_col = jnp.sum(jnp.where(pick, dot(spread, p_on.astype(BF), NN), 0.0), axis=1, keepdims=True)
    pick = pick.astype(F32).astype(BF)
    pick_ref[...] = pick
    tokp[0:WID, :] = tok_ref[...]
    tokp[WID:PAD, :] = jnp.zeros((PAD - WID, TOK), BF)
    for q in range(3):
        val = dot(pick, tokp[256 * q : 256 * q + 256, :], NT)
        if q == 2:
            val = jnp.where(iota((ROWS, 256), 1) == PROB - 512, p_col, val)
        val = val.astype(BF)
        for j in (2 * q, 2 * q + 1):
            tile = val[:, 128 * (j - 2 * q) : 128 * (j - 2 * q) + 128]
            send_ref[:, MAIN * j : MAIN * j + MAIN, :] = tile[:MROWS].reshape(OWNERS, MAIN, 128)
            rest[:, 128 * j : 128 * j + 128] = tile[MROWS:]
    pack_rest(rest, send_ref, PAD)


def dispatch_d_body(t_ref, pick_ref, own_ref, below_ref, above_ref, far_a_ref, far_b_ref, send_ref, full, rest):
    t = t_ref[0]

    def put(side, ref, off, rows):
        j = lax.rem(t + side, SIDES)
        full[pl.ds(pl.multiple_of(WID * j + off, 16), rows), :] = ref[...]

    put(0, own_ref, 0, WID)
    put(3, below_ref, 0, WID)
    put(1, above_ref, 0, WID)
    put(2, far_a_ref, 0, 368)
    put(2, far_b_ref, 368, WID - 368)
    full[FEAT:3072, :] = jnp.zeros((3072 - FEAT, TOK), BF)
    pick = pick_ref[...]
    for q in range(12):
        val = dot(pick, full[256 * q : 256 * q + 256, :], NT).astype(BF)
        for j in (2 * q, 2 * q + 1):
            if j < tiles_of(FPAD):
                tile = val[:, 128 * (j - 2 * q) : 128 * (j - 2 * q) + 128]
                send_ref[:, MAIN * j : MAIN * j + MAIN, :] = tile[:MROWS].reshape(OWNERS, MAIN, 128)
                rest[:, 128 * j : 128 * j + 128] = tile[MROWS:]
    pack_rest(rest, send_ref, FPAD)


def turn_body(t_ref, w_ref, out_ref):
    t = t_ref[0]
    pieces = [w_ref[:, WID * j : WID * j + WID] for j in range(SIDES)]
    for k in range(SIDES):
        j = lax.rem(t + k, SIDES)
        piece = jnp.where(j == 0, pieces[0], jnp.where(j == 1, pieces[1], jnp.where(j == 2, pieces[2], pieces[3])))
        out_ref[k, :, 0:WID] = piece
        out_ref[k, :, WID:PAD] = jnp.zeros((piece.shape[0], PAD - WID), BF)


CHUNKS = ((0, 256), (256, 256), (512, WID - 512))


def copies(pairs, sems):
    out = []
    for n, (src, dst) in enumerate(pairs):
        copy = pltpu.make_async_copy(src, dst, sems.at[n])
        copy.start()
        out.append(copy)
    return out


def gate_up_body(*refs):
    x_refs, w_refs, (act_out, mid_out, x_out), (w, act, mid, x, in_sems, out_sems) = refs[:7], refs[7:9], refs[9:12], refs[12:]
    loads = copies(
        [(w_refs[n].at[:, lo : lo + size, :], w.at[n, :, lo : lo + size, :]) for lo, size in CHUNKS for n in range(2)], in_sems
    )

    def keep(side):
        def store(row, lane, value):
            x[side, row : row + value.shape[0], lane : lane + 128] = value

        return store

    unpack(x_refs[0], PAD, keep(0))
    for n, side in enumerate((3, 1, 2)):
        unpack(x_refs[2 * n + 1], PAD, keep(side), 0)
        unpack(x_refs[2 * n + 2], PAD, keep(side), OWNERS // 2)
    stores = [pltpu.make_async_copy(x, x_out, out_sems.at[6])]
    stores[0].start()
    for c, (lo, size) in enumerate(CHUNKS):
        loads[2 * c].wait()
        loads[2 * c + 1].wait()
        gate, up1 = (sum(dot(x[k], w[n, k, lo : lo + size, :], NT) for k in range(SIDES)) for n in range(2))
        up1 = up1 + 1.0
        sig = 1.0 / (1.0 + jnp.exp(-SWISH_SLOPE * gate))
        glu = gate * sig
        act[:, lo : lo + size] = (glu * up1).astype(BF)
        mid[0, :, lo : lo + size] = up1 * (sig + SWISH_SLOPE * glu * (1.0 - sig))
        mid[1, :, lo : lo + size] = glu
        if c == 2:
            tile = x[0, :, 640:768].astype(F32)
            p_col = jnp.sum(jnp.where(iota((ROWS, 128), 1) == PROB - 640, tile, 0.0), axis=1, keepdims=True)
            mid[0, :, WID:PAD] = jnp.broadcast_to(p_col, (ROWS, PAD - WID))
            mid[1, :, WID:PAD] = jnp.zeros((ROWS, PAD - WID), F32)
            act[:, WID:PAD] = jnp.zeros((ROWS, PAD - WID), BF)
        cols = slice(lo, lo + 256)
        for n, (src, dst) in enumerate(((act.at[:, cols], act_out.at[:, cols]), (mid.at[:, :, cols], mid_out.at[:, :, cols]))):
            stores.append(pltpu.make_async_copy(src, dst, out_sems.at[2 * c + n]))
            stores[-1].start()
    for copy in stores:
        copy.wait()


def back_body(
    got_hbm, wd_hbm, act_hbm, mid_hbm, wg_hbm, wu_hbm,
    d_out, gg_ref, gu_ref, prob_ref, p_ref, a_ref, b_ref,
    got, wd, act, mid, wg, wu, d, sems, out_sem,
):
    got_loads = copies([(got_hbm.at[8 * i : 8 * i + 8], got.at[8 * i : 8 * i + 8]) for i in range(4)], sems)
    loads = copies(
        [(wd_hbm.at[lo : lo + size, :], wd.at[lo : lo + size, :]) for lo, size in CHUNKS]
        + [(mid_hbm, mid), (act_hbm, act), (wg_hbm.at[2], wg), (wu_hbm.at[2], wu)],
        sems.at[4:],
    )

    def store(row, lane, value):
        width = min(128, FEAT - lane)
        d[row : row + value.shape[0], lane : lane + width] = value[:, :width]

    for i in range(4):
        got_loads[i].wait()
        unpack(got.at[8 * i : 8 * i + 8], FPAD, store, 8 * i)
    keep_d = pltpu.make_async_copy(d, d_out, out_sem)
    keep_d.start()
    total = jnp.zeros((ROWS, 1), F32)
    for c, (lo, size) in enumerate(CHUNKS):
        loads[c].wait()
        down_back = dot(d[...], wd[lo : lo + size, :], NT)
        if c == 0:
            loads[3].wait()
            loads[4].wait()
            p_col = mid[0, :, 640:768][:, WID - 640 : WID - 639]
            p_ref[...] = p_col
        delta = p_col * down_back
        gg_ref[:, lo : lo + size] = (delta * mid[0, :, lo : lo + size]).astype(BF)
        gu_ref[:, lo : lo + size] = (delta * mid[1, :, lo : lo + size]).astype(BF)
        total = total + jnp.sum(act[:, lo : lo + size].astype(F32) * down_back, axis=1, keepdims=True)
    prob_ref[...] = jnp.where(iota((ROWS, 128), 1) == PROB - 640, total, 0.0)
    loads[5].wait()
    loads[6].wait()
    left, right = dx_of(gg_ref[...], gu_ref[...], wg[...], wu[...], prob_ref[...])
    right = split_prob(right)
    put_rows(a_ref, left[:HALF], right[:HALF])
    put_rows(b_ref, left[HALF:], right[HALF:])
    keep_d.wait()


def split_prob(tile):
    lane = iota(tile.shape, 1)
    total = jnp.sum(jnp.where(lane == PROB - 640, tile, 0.0), axis=1, keepdims=True)
    high = total.astype(BF).astype(F32)
    return jnp.where(lane == PROB - 640, high, jnp.where(lane == PROB - 639, total - high, tile))


def join_prob(tile):
    lane = iota(tile.shape, 1)
    total = jnp.sum(jnp.where((lane == PROB - 640) | (lane == PROB - 639), tile, 0.0), axis=1, keepdims=True)
    return jnp.where(lane == PROB - 640, total, jnp.where(lane == PROB - 639, 0.0, tile))


HALF = ROWS // 2


def dx_of(gg, gu, wg, wu, prob):
    val = dot(gg, wg, NN) + dot(gu, wu, NN)
    return val[:, :640], val[:, 640:768] + prob


def put_rows(ref, left, right):
    ref[:, 0:640] = left.astype(ref.dtype)
    ref[:, 640:768] = right.astype(ref.dtype)


def near_dx_body(gg_ref, gu_ref, wga_ref, wua_ref, wgb_ref, wub_ref, prob_ref, send_a, send_b, keep_a, keep_b):
    gg, gu, prob = gg_ref[...], gu_ref[...], prob_ref[...]
    left, right = dx_of(gg, gu, wga_ref[0], wua_ref[0], prob)
    put_rows(send_a, left[HALF:], split_prob(right)[HALF:])
    put_rows(keep_a, left[:HALF], right[:HALF])
    left, right = dx_of(gg, gu, wgb_ref[0], wub_ref[0], prob)
    put_rows(send_b, left[:HALF], split_prob(right)[:HALF])
    put_rows(keep_b, left[HALF:], right[HALF:])


def own_dx_body(gg_ref, gu_ref, wg_ref, wu_ref, prob_ref, out_ref):
    put_rows(out_ref, *dx_of(gg_ref[...], gu_ref[...], wg_ref[0], wu_ref[0], prob_ref[...]))


def relay_body(keep_a, came_a, keep_b, came_b, out_a, out_b):
    for keep, came, out in ((keep_a, came_a, out_a), (keep_b, came_b, out_b)):
        left = keep[:, 0:640] + came[:, 0:640].astype(F32)
        put_rows(out, left, split_prob(keep[:, 640:768] + join_prob(came[:, 640:768].astype(F32))))


def sum_body(own_ref, below_a, below_b, above_a, above_b, send_ref, rest):
    for j in range(tiles_of(PAD)):
        cols = slice(128 * j, 128 * j + 128)
        tile = [
            own_ref[lo : lo + HALF, cols] + below[:, cols].astype(F32) + above[:, cols].astype(F32)
            for lo, below, above in ((0, below_a, above_a), (HALF, below_b, above_b))
        ]
        tile = jnp.concatenate(tile, axis=0)
        if j == 5:
            tile = join_prob(tile)
        tile = tile.astype(BF)
        send_ref[:, MAIN * j : MAIN * j + MAIN, :] = tile[:MROWS].reshape(OWNERS, MAIN, 128)
        rest[:, cols] = tile[MROWS:]
    pack_rest(rest, send_ref, PAD)


def combine_body(back_ref, pick_ref, ids_ref, map_ref, dx_ref, dp_ref, rows):
    def store(row, lane, value):
        rows[row : row + value.shape[0], lane : lane + 128] = value

    unpack(back_ref, PAD, store)
    pick = pick_ref[...]
    dx_ref[...] = dot(rows[...], pick, TN)[:WID].astype(BF)
    tile = rows[:, 640:768].astype(F32)
    p_col = jnp.sum(jnp.where(iota((ROWS, 128), 1) == PROB - 640, tile, 0.0), axis=1, keepdims=True)
    spread = (row_owner((OWNERS, ROWS), 1) == iota((OWNERS, ROWS), 0)).astype(F32).astype(BF)
    per_owner = dot(spread, (pick.astype(F32) * p_col).astype(BF), NN)
    hits = hits_of(ids_ref, map_ref)
    for k in range(TOP):
        dp_ref[k : k + 1, :] = jnp.sum(jnp.where(hits[k], per_owner, 0.0), axis=0, keepdims=True).astype(BF)


def grad_pair_body(t_ref, x_ref, gg_ref, gu_ref, gate_ref, up_ref):
    t = t_ref[0]
    for j in range(SIDES):
        k = lax.rem(j - t + SIDES, SIDES)
        x = x_ref[pl.ds(k, 1)][0]
        for src, out in ((gg_ref, gate_ref), (gu_ref, up_ref)):
            out[:, WID * j : WID * j + WID] = dot(src[...], x, TN).astype(BF)[:, :WID]


def down_body(d_ref, act_ref, p_ref, out_ref, scaled):
    @pl.when(pl.program_id(0) == 0)
    def _():
        scaled[...] = (d_ref[...].astype(F32) * p_ref[...]).astype(BF)

    out_ref[...] = dot(act_ref[...], scaled[...], TN).astype(BF)


def turn(w, t):
    return call(
        turn_body,
        struct((SIDES, WID, PAD)),
        grid=(3,),
        in_specs=[sm(), pl.BlockSpec((240, FEAT), lambda i: (i, 0))],
        out_specs=pl.BlockSpec((SIDES, 240, PAD), lambda i: (0, i, 0)),
        vmem=60,
    )(t, w)


def hbm():
    return pl.BlockSpec(memory_space=pltpu.HBM)


def dma(*shape):
    return pltpu.SemaphoreType.DMA(shape)


def whole(shape):
    return pl.BlockSpec(shape, lambda i: (0,) * len(shape))


def hold(*values):
    return lax.optimization_barrier(values)


def shards(tokens, out_grad, route_probs, expert_ids, placement_map, w_gate, w_up, w_down):
    above = [((i + 1) % SIDES, i) for i in range(SIDES)]
    below = [((i - 1) % SIDES, i) for i in range(SIDES)]

    def from_above(value):
        return lax.ppermute(value, "tensor", above)

    def from_below(value):
        return lax.ppermute(value, "tensor", below)

    t = lax.axis_index("tensor").astype(jnp.int32).reshape(1)
    tok_t, d_t, ids_t, prob_t = tokens.T, out_grad.T, expert_ids.T, route_probs.T
    pmap = placement_map.reshape(1, -1)
    wg_t, wu_t, wd = w_gate[0].T, w_up[0].T, w_down[0]
    bx = block_rows(PAD)
    bd = block_rows(FPAD)
    t, d_t = hold(t, d_t)
    d_above, d_below = from_above(d_t), from_below(d_t)
    send_x, pick = call(
        dispatch_x_body,
        (struct((OWNERS, bx, 128)), struct((ROWS, TOK))),
        in_specs=[vm()] * 4,
        out_specs=(vm(), vm()),
        scratch_shapes=[pltpu.VMEM((PAD, TOK), BF), pltpu.VMEM((ROWS - MROWS, PAD), BF)],
        flops=10**9,
        vmem=60,
    )(ids_t, prob_t, pmap, tok_t)
    got_x = lax.all_to_all(send_x, "dp", 0, 0, tiled=True)
    d_far_a, d_far_b = from_below(d_below[:368]), from_above(d_above[368:])
    wg = turn(wg_t, t)
    wu = turn(wu_t, t)
    x_a, x_b = got_x[: OWNERS // 2], got_x[OWNERS // 2 :]
    x_below_a, x_above_b = from_below(x_a), from_above(x_b)
    x_below_b, x_above_a = from_below(x_b), from_above(x_a)
    send_d = call(
        dispatch_d_body,
        struct((OWNERS, bd, 128)),
        in_specs=[sm()] + [vm()] * 6,
        out_specs=vm(),
        scratch_shapes=[pltpu.VMEM((3072, TOK), BF), pltpu.VMEM((ROWS - MROWS, FPAD), BF)],
        flops=2 * 10**9,
        vmem=60,
    )(t, pick, d_t, d_below, d_above, d_far_a, d_far_b)
    got_d = lax.all_to_all(send_d, "dp", 0, 0, tiled=True)
    x_far_a, x_far_b = from_below(x_below_a), from_above(x_above_b)
    act_spec = pl.BlockSpec((ROWS, 256), lambda i: (0, i))
    row_spec = pl.BlockSpec((256, FEAT), lambda i: (i, 0))
    mid = struct((ROWS, WID))
    half, half32 = struct((HALF, PAD)), struct((HALF, PAD), F32)
    act, fgu, x_rel = call(
        gate_up_body,
        (struct((ROWS, PAD)), struct((2, ROWS, PAD), F32), struct((SIDES, ROWS, PAD))),
        in_specs=[vm()] * 7 + [hbm()] * 2,
        out_specs=(hbm(),) * 3,
        scratch_shapes=[
            pltpu.VMEM((2, SIDES, WID, PAD), BF),
            pltpu.VMEM((ROWS, PAD), BF),
            pltpu.VMEM((2, ROWS, PAD), F32),
            pltpu.VMEM((SIDES, ROWS, PAD), BF),
            dma(6),
            dma(7),
        ],
        flops=5 * 10**9,
        vmem=GATE_VMEM,
    )(got_x, x_below_a, x_below_b, x_above_a, x_above_b, x_far_a, x_far_b, wg, wu)
    d_rows, gg, gu, prob, p_col, part_a, part_b = call(
        back_body,
        (struct((ROWS, FEAT)), mid, mid, struct((ROWS, 128), F32), struct((ROWS, 1), F32), half, half),
        in_specs=[hbm()] * 6,
        out_specs=(hbm(),) + (vm(),) * 6,
        scratch_shapes=[
            pltpu.VMEM((OWNERS, bd, 128), BF),
            pltpu.VMEM((WID, FEAT), BF),
            pltpu.VMEM((ROWS, PAD), BF),
            pltpu.VMEM((2, ROWS, PAD), F32),
            pltpu.VMEM((WID, PAD), BF),
            pltpu.VMEM((WID, PAD), BF),
            pltpu.VMEM((ROWS, FEAT), BF),
            dma(11),
            pltpu.SemaphoreType.DMA,
        ],
        flops=4 * 10**9,
        vmem=BACK_VMEM,
    )(got_d, wd, act, fgu, wg, wu)
    came_a, came_b = from_below(part_a), from_above(part_b)
    side = lambda k: pl.BlockSpec((1, WID, PAD), lambda i: (k, 0, 0))
    acts = [whole((ROWS, WID))] * 2
    tail = [whole((ROWS, 128))]
    send_a, send_b, keep_a, keep_b = call(
        near_dx_body,
        (half, half, half32, half32),
        grid=(1,),
        in_specs=acts + [side(1), side(1), side(3), side(3)] + tail,
        out_specs=(whole((HALF, PAD)),) * 4,
        flops=24 * 10**8,
        vmem=20,
    )(gg, gu, wg, wu, wg, wu, prob)
    below_b, above_a = from_below(send_a), from_above(send_b)
    own = call(
        own_dx_body,
        struct((ROWS, PAD), F32),
        grid=(1,),
        in_specs=acts + [side(0), side(0)] + tail,
        out_specs=whole((ROWS, PAD)),
        flops=12 * 10**8,
        vmem=20,
    )(gg, gu, wg, wu, prob)
    pass_a, pass_b = call(relay_body, (half, half), in_specs=[vm()] * 4, out_specs=(vm(), vm()), vmem=10)(
        keep_a, came_a, keep_b, came_b
    )
    below_a, above_b = from_below(pass_a), from_above(pass_b)
    gate_grad, up_grad = call(
        grad_pair_body,
        (struct((WID, FEAT)), struct((WID, FEAT))),
        grid=(3,),
        in_specs=[sm(), whole((SIDES, ROWS, PAD)), act_spec, act_spec],
        out_specs=(row_spec, row_spec),
        flops=5 * 10**9,
        vmem=20,
    )(t, x_rel, gg, gu)
    below_a, above_b, gate_grad, up_grad = hold(below_a, above_b, gate_grad, up_grad)
    send_back = call(
        sum_body,
        struct((OWNERS, bx, 128)),
        in_specs=[vm()] * 5,
        out_specs=vm(),
        scratch_shapes=[pltpu.VMEM((ROWS - MROWS, PAD), BF)],
        vmem=10,
    )(own, below_a, below_b, above_a, above_b)
    back = lax.all_to_all(send_back, "dp", 0, 0, tiled=True)
    down_grad = call(
        down_body,
        struct((WID, FEAT)),
        grid=(3,),
        in_specs=[whole((ROWS, FEAT)), act_spec, whole((ROWS, 1))],
        out_specs=row_spec,
        scratch_shapes=[pltpu.VMEM((ROWS, FEAT), BF)],
        flops=3 * 10**9,
        vmem=20,
    )(d_rows, act, p_col)
    dx_t, dp_t = call(
        combine_body,
        (struct((WID, TOK)), struct((TOP, TOK))),
        in_specs=[vm()] * 4,
        out_specs=(vm(), vm()),
        scratch_shapes=[pltpu.VMEM((ROWS, PAD), BF)],
        flops=10**9,
        vmem=10,
    )(back, pick, ids_t, pmap)
    return dx_t.T, gate_grad.T[None], up_grad.T[None], down_grad[None], dp_t.T


def solution(mesh):
    in_specs = (
        P("dp", "tensor"),
        P("dp", "tensor"),
        P("dp", None),
        P("dp", None),
        P(),
        P("dp", None, "tensor"),
        P("dp", None, "tensor"),
        P("dp", "tensor", None),
    )
    out_specs = (
        P("dp", "tensor"),
        P("dp", None, "tensor"),
        P("dp", None, "tensor"),
        P("dp", "tensor", None),
        P("dp", None),
    )

    return jax.shard_map(shards, mesh=mesh, in_specs=in_specs, out_specs=out_specs, check_vma=False)
```

```python
import jax
import jax.numpy as jnp
from jax import lax
from jax.experimental import pallas as pl
from jax.experimental.pallas import tpu as pltpu
from jax.sharding import PartitionSpec as P


SWISH_SLOPE = 1.702
EXP_OWN = 4
OWNERS = 32
CAP = 18
MAIN = 16
ROWS = OWNERS * CAP
MROWS = OWNERS * MAIN
TOK = 384
TOP = 4
WID = 720
PAD = 768
FEAT = 2880
FPAD = 2944
SIDES = 4
GATE_VMEM = 58
TURN_VMEM = 59
NEAR_VMEM = 20
SEND_VMEM = 44
BACK_VMEM = 52
PROB = 720

BF = jnp.bfloat16
F32 = jnp.float32
NT = (((1,), (1,)), ((), ()))
TN = (((0,), (0,)), ((), ()))
NN = (((1,), (0,)), ((), ()))


def dot(a, b, dims):
    return lax.dot_general(a, b, dims, preferred_element_type=F32)


def call(body, out_shape, **kw):
    params = pltpu.CompilerParams(vmem_limit_bytes=kw.pop("vmem", 8) << 20, **({"dimension_semantics": ("arbitrary",)} if "grid" in kw else {}))
    flops = kw.pop("flops", 0)
    nbytes = kw.pop("nbytes", 4 << 20)
    return pl.pallas_call(
        body,
        out_shape=out_shape,
        compiler_params=params,
        cost_estimate=pl.CostEstimate(flops=flops, bytes_accessed=nbytes, transcendentals=0),
        **kw,
    )


def struct(shape, dtype=BF):
    return jax.ShapeDtypeStruct(shape, dtype)


def vm():
    return pl.BlockSpec(memory_space=pltpu.VMEM)


def sm():
    return pl.BlockSpec(memory_space=pltpu.SMEM)


def iota(shape, dim):
    return lax.broadcasted_iota(jnp.int32, shape, dim)


def swap_matrix():
    r, q = iota((128, 128), 0), iota((128, 128), 1)
    return (((r >> 4) == ((q >> 1) & 7)) & ((q >> 4) == ((r >> 1) & 7)) & ((r & 1) == (q & 1))).astype(BF)


def tiles_of(width):
    return width // 128


def block_rows(width):
    t = tiles_of(width)
    return MAIN * t + 16 * ((t + 7) // 8)


def pack_rest(rest, out_ref, width):
    t = tiles_of(width)
    swap = swap_matrix()
    for a in range((t + 7) // 8):
        for i in range(OWNERS // 8):
            parts = [
                rest[16 * i : 16 * i + 16, 128 * j : 128 * j + 128] if j < t else jnp.zeros((16, 128), BF)
                for j in range(8 * a, 8 * a + 8)
            ]
            turned = dot(swap, jnp.concatenate(parts, axis=0), NN).astype(BF)
            out_ref[8 * i : 8 * i + 8, MAIN * t + 16 * a : MAIN * t + 16 * a + 16, :] = turned.reshape(8, 16, 128)


def unpack(ref, width, store, first=0):
    t = tiles_of(width)
    peers = ref.shape[0]
    for j in range(t):
        store(MAIN * first, 128 * j, ref[:, MAIN * j : MAIN * j + MAIN, :].reshape(MAIN * peers, 128))
    swap = swap_matrix()
    for a in range((t + 7) // 8):
        for i in range(peers // 8):
            block = ref[8 * i : 8 * i + 8, MAIN * t + 16 * a : MAIN * t + 16 * a + 16, :].reshape(128, 128)
            turned = dot(swap, block, NN).astype(BF)
            for b in range(8):
                j = 8 * a + b
                if j < t:
                    store(MROWS + 2 * first + 16 * i, 128 * j, turned[16 * b : 16 * b + 16])


def row_owner(shape, dim):
    r = iota(shape, dim)
    return jnp.where(r < MROWS, r >> 4, (r - MROWS) >> 1)


def row_slot(shape, dim):
    r = iota(shape, dim)
    return jnp.where(r < MROWS, r & 15, MAIN + (r & 1))


def hits_of(ids_ref, map_ref):
    experts = map_ref.shape[1]
    eq = map_ref[...] == EXP_OWN * iota((OWNERS, experts), 0)
    held = jnp.sum(jnp.where(eq, iota((OWNERS, experts), 1), 0), axis=1, keepdims=True)
    return [ids_ref[k : k + 1, :] == held for k in range(TOP)]


def dispatch_x_body(ids_ref, prob_ref, map_ref, tok_ref, send_ref, pick_ref, tokp, rest):
    hits = hits_of(ids_ref, map_ref)
    probs = prob_ref[...].astype(F32)
    named = hits[0] | hits[1] | hits[2] | hits[3]
    p_on = jnp.zeros((OWNERS, TOK), F32)
    for k in range(TOP):
        p_on = jnp.where(hits[k], probs[k : k + 1, :], p_on)
    upper = (iota((TOK, TOK), 0) < iota((TOK, TOK), 1)).astype(F32).astype(BF)
    rank = dot(named.astype(F32).astype(BF), upper, NN)
    key = jnp.where(named, rank, -1.0).astype(BF)
    spread = (row_owner((ROWS, OWNERS), 0) == iota((ROWS, OWNERS), 1)).astype(F32).astype(BF)
    pick = dot(spread, key, NN) == row_slot((ROWS, TOK), 0).astype(F32)
    p_col = jnp.sum(jnp.where(pick, dot(spread, p_on.astype(BF), NN), 0.0), axis=1, keepdims=True)
    pick = pick.astype(F32).astype(BF)
    pick_ref[...] = pick
    tokp[0:WID, :] = tok_ref[...]
    tokp[WID:PAD, :] = jnp.zeros((PAD - WID, TOK), BF)
    for q in range(3):
        val = dot(pick, tokp[256 * q : 256 * q + 256, :], NT)
        if q == 2:
            val = jnp.where(iota((ROWS, 256), 1) == PROB - 512, p_col, val)
        val = val.astype(BF)
        for j in (2 * q, 2 * q + 1):
            tile = val[:, 128 * (j - 2 * q) : 128 * (j - 2 * q) + 128]
            send_ref[:, MAIN * j : MAIN * j + MAIN, :] = tile[:MROWS].reshape(OWNERS, MAIN, 128)
            rest[:, 128 * j : 128 * j + 128] = tile[MROWS:]
    pack_rest(rest, send_ref, PAD)


def dispatch_d_body(t_ref, pick_ref, own_ref, below_ref, above_ref, far_a_ref, far_b_ref, send_ref, full, rest):
    t = t_ref[0]

    def put(side, ref, off, rows):
        j = lax.rem(t + side, SIDES)
        full[pl.ds(pl.multiple_of(WID * j + off, 16), rows), :] = ref[...]

    put(0, own_ref, 0, WID)
    put(3, below_ref, 0, WID)
    put(1, above_ref, 0, WID)
    put(2, far_a_ref, 0, 368)
    put(2, far_b_ref, 368, WID - 368)
    full[FEAT:3072, :] = jnp.zeros((3072 - FEAT, TOK), BF)
    pick = pick_ref[...]
    for q in range(12):
        val = dot(pick, full[256 * q : 256 * q + 256, :], NT).astype(BF)
        for j in (2 * q, 2 * q + 1):
            if j < tiles_of(FPAD):
                tile = val[:, 128 * (j - 2 * q) : 128 * (j - 2 * q) + 128]
                send_ref[:, MAIN * j : MAIN * j + MAIN, :] = tile[:MROWS].reshape(OWNERS, MAIN, 128)
                rest[:, 128 * j : 128 * j + 128] = tile[MROWS:]
    pack_rest(rest, send_ref, FPAD)


def turn_body(t_ref, w_ref, out_ref):
    t = t_ref[0]
    pieces = [w_ref[:, WID * j : WID * j + WID] for j in range(SIDES)]
    for k in range(SIDES):
        j = lax.rem(t + k, SIDES)
        piece = jnp.where(j == 0, pieces[0], jnp.where(j == 1, pieces[1], jnp.where(j == 2, pieces[2], pieces[3])))
        out_ref[k, :, 0:WID] = piece
        out_ref[k, :, WID:PAD] = jnp.zeros((piece.shape[0], PAD - WID), BF)


CHUNKS = ((0, 256), (256, 256), (512, WID - 512))


def copies(pairs, sems):
    out = []
    for n, (src, dst) in enumerate(pairs):
        copy = pltpu.make_async_copy(src, dst, sems.at[n])
        copy.start()
        out.append(copy)
    return out


def gate_up_body(*refs):
    x_refs, w_refs, (act_out, mid_out, x_out), (got, w, act, mid, x, got_sems, in_sems, out_sems) = refs[:7], refs[7:9], refs[9:12], refs[12:]
    peers = [slice(0, OWNERS)] + [slice(0, OWNERS // 2), slice(OWNERS // 2, OWNERS)] * 3
    sides = [0, 3, 3, 1, 1, 2, 2]
    blocks = [got.at[side, part] for side, part in zip(sides, peers)]
    got_loads = copies(list(zip(x_refs, blocks)), got_sems)
    pairs = [(w_refs[n].at[:, lo : lo + size, :], w.at[n, :, lo : lo + size, :]) for lo, size in CHUNKS for n in range(2)]
    loads = copies(pairs[:2], in_sems)

    def keep(side):
        def store(row, lane, value):
            x[side, row : row + value.shape[0], lane : lane + 128] = value

        return store

    for n, (side, part) in enumerate(zip(sides, peers)):
        got_loads[n].wait()
        unpack(blocks[n], PAD, keep(side), part.start)
    loads += copies(pairs[2:], in_sems.at[2:])
    stores = [pltpu.make_async_copy(x, x_out, out_sems.at[6])]
    stores[0].start()
    for c, (lo, size) in enumerate(CHUNKS):
        loads[2 * c].wait()
        loads[2 * c + 1].wait()
        gate, up1 = (sum(dot(x[k], w[n, k, lo : lo + size, :], NT) for k in range(SIDES)) for n in range(2))
        up1 = up1 + 1.0
        sig = 1.0 / (1.0 + jnp.exp(-SWISH_SLOPE * gate))
        glu = gate * sig
        act[:, lo : lo + size] = (glu * up1).astype(BF)
        mid[0, :, lo : lo + size] = (up1 * (sig + SWISH_SLOPE * glu * (1.0 - sig))).astype(BF)
        mid[1, :, lo : lo + size] = glu.astype(BF)
        if c == 2:
            tile = x[0, :, 640:768].astype(F32)
            p_col = jnp.sum(jnp.where(iota((ROWS, 128), 1) == PROB - 640, tile, 0.0), axis=1, keepdims=True)
            act[:, WID:PAD] = jnp.broadcast_to(p_col, (ROWS, PAD - WID)).astype(BF)
            mid[:, :, WID:PAD] = jnp.zeros((2, ROWS, PAD - WID), BF)
        cols = slice(lo, lo + 256)
        for n, (src, dst) in enumerate(((act.at[:, cols], act_out.at[:, cols]), (mid.at[:, :, cols], mid_out.at[:, :, cols]))):
            stores.append(pltpu.make_async_copy(src, dst, out_sems.at[2 * c + n]))
            stores[-1].start()
    for copy in stores:
        copy.wait()


def back_body(
    got_hbm, wd_hbm, act_hbm, mid_hbm, wg_hbm, wu_hbm,
    gg_out, gu_out, prob_ref, a_ref, b_ref,
    got, wd, act, mid, g, w, d, got_sems, sems, out_sems,
):
    eights = [slice(8 * i, 8 * i + 8) for i in range(OWNERS // 8)]
    got_loads = copies([(got_hbm.at[part], got.at[part]) for part in eights], got_sems)
    pairs = []
    for lo, size in CHUNKS:
        cols = slice(lo, lo + 256)
        pairs += [
            (wd_hbm.at[lo : lo + size, :], wd.at[lo : lo + size, :]),
            (mid_hbm.at[:, :, cols], mid.at[:, :, cols]),
        ]
        if lo == 0:
            pairs.append((act_hbm, act))
    pairs += [(ref.at[2], w.at[PAD * n : PAD * n + WID, :]) for n, ref in enumerate((wg_hbm, wu_hbm))]
    loads = copies(pairs[:3], sems)

    def store(row, lane, value):
        width = min(128, FEAT - lane)
        d[row : row + value.shape[0], lane : lane + width] = value[:, :width]

    for part, copy in zip(eights, got_loads):
        copy.wait()
        unpack(got.at[part], FPAD, store, part.start)
    loads += copies(pairs[3:], sems.at[3:])
    for n in range(2):
        w[PAD * n + WID : PAD * n + PAD, :] = jnp.zeros((PAD - WID, PAD), BF)
        g[:, PAD * n + WID : PAD * n + PAD] = jnp.zeros((ROWS, PAD - WID), BF)
    total = jnp.zeros((ROWS, 1), F32)
    for c, (lo, size) in enumerate(CHUNKS):
        wait = loads[:3] if c == 0 else loads[2 * c + 1 : 2 * c + 3]
        wait[0].wait()
        down_back = dot(d[...], wd[lo : lo + size, :], NT)
        for copy in wait[1:]:
            copy.wait()
        if c == 0:
            p_col = act[:, 640:768].astype(F32)[:, PROB - 640 : PROB - 639]
        delta = p_col * down_back
        g[:, lo : lo + size] = (delta * mid[0, :, lo : lo + size]).astype(BF)
        g[:, PAD + lo : PAD + lo + size] = (delta * mid[1, :, lo : lo + size]).astype(BF)
        total = total + jnp.sum(act[:, lo : lo + size].astype(F32) * down_back, axis=1, keepdims=True)
    stores = copies([(g.at[:, 0:PAD], gg_out), (g.at[:, PAD : 2 * PAD], gu_out)], out_sems)
    prob = jnp.where(iota((ROWS, 128), 1) == PROB - 640, total, 0.0)
    prob_ref[...] = prob
    loads[7].wait()
    loads[8].wait()
    val = dot(g[...], w[...], NN)
    left, right = val[:, :640], split_prob(val[:, 640:768] + prob)
    put_rows(a_ref, left[:HALF], right[:HALF])
    put_rows(b_ref, left[HALF:], right[HALF:])
    for copy in stores:
        copy.wait()


def split_prob(tile):
    lane = iota(tile.shape, 1)
    total = jnp.sum(jnp.where(lane == PROB - 640, tile, 0.0), axis=1, keepdims=True)
    high = total.astype(BF).astype(F32)
    return jnp.where(lane == PROB - 640, high, jnp.where(lane == PROB - 639, total - high, tile))


def join_prob(tile):
    lane = iota(tile.shape, 1)
    total = jnp.sum(jnp.where((lane == PROB - 640) | (lane == PROB - 639), tile, 0.0), axis=1, keepdims=True)
    return jnp.where(lane == PROB - 640, total, jnp.where(lane == PROB - 639, 0.0, tile))


HALF = ROWS // 2


def dx_of(gg, gu, wg, wu, prob):
    val = dot(gg[:, :WID], wg, NN) + dot(gu[:, :WID], wu, NN)
    return val[:, :640], val[:, 640:768] + prob


def put_rows(ref, left, right):
    ref[:, 0:640] = left.astype(ref.dtype)
    ref[:, 640:768] = right.astype(ref.dtype)


def near_dx_body(gg_ref, gu_ref, wga_ref, wua_ref, wgb_ref, wub_ref, prob_ref, send_a, send_b, keep_a, keep_b):
    gg, gu, prob = gg_ref[...], gu_ref[...], prob_ref[...]
    left, right = dx_of(gg, gu, wga_ref[0], wua_ref[0], prob)
    put_rows(send_a, left[HALF:], split_prob(right)[HALF:])
    put_rows(keep_a, left[:HALF], right[:HALF])
    left, right = dx_of(gg, gu, wgb_ref[0], wub_ref[0], prob)
    put_rows(send_b, left[:HALF], split_prob(right)[:HALF])
    put_rows(keep_b, left[HALF:], right[HALF:])


def own_dx_body(gg_ref, gu_ref, wg_ref, wu_ref, prob_ref, out_ref):
    put_rows(out_ref, *dx_of(gg_ref[...], gu_ref[...], wg_ref[0], wu_ref[0], prob_ref[...]))


def relay_body(keep_a, came_a, keep_b, came_b, out_a, out_b):
    for keep, came, out in ((keep_a, came_a, out_a), (keep_b, came_b, out_b)):
        left = keep[:, 0:640] + came[:, 0:640].astype(F32)
        put_rows(out, left, split_prob(keep[:, 640:768] + join_prob(came[:, 640:768].astype(F32))))


def sum_body(own_ref, below_a, below_b, above_a, above_b, send_ref, rest):
    for j in range(tiles_of(PAD)):
        cols = slice(128 * j, 128 * j + 128)
        tile = [
            own_ref[lo : lo + HALF, cols] + below[:, cols].astype(F32) + above[:, cols].astype(F32)
            for lo, below, above in ((0, below_a, above_a), (HALF, below_b, above_b))
        ]
        tile = jnp.concatenate(tile, axis=0)
        if j == 5:
            tile = join_prob(tile)
        tile = tile.astype(BF)
        send_ref[:, MAIN * j : MAIN * j + MAIN, :] = tile[:MROWS].reshape(OWNERS, MAIN, 128)
        rest[:, cols] = tile[MROWS:]
    pack_rest(rest, send_ref, PAD)


def combine_body(back_ref, pick_ref, ids_ref, map_ref, dx_ref, dp_ref, rows):
    def store(row, lane, value):
        rows[row : row + value.shape[0], lane : lane + 128] = value

    unpack(back_ref, PAD, store)
    pick = pick_ref[...]
    dx_ref[...] = dot(rows[...], pick, TN)[:WID].astype(BF)
    tile = rows[:, 640:768].astype(F32)
    p_col = jnp.sum(jnp.where(iota((ROWS, 128), 1) == PROB - 640, tile, 0.0), axis=1, keepdims=True)
    spread = (row_owner((OWNERS, ROWS), 1) == iota((OWNERS, ROWS), 0)).astype(F32).astype(BF)
    per_owner = dot(spread, (pick.astype(F32) * p_col).astype(BF), NN)
    hits = hits_of(ids_ref, map_ref)
    for k in range(TOP):
        dp_ref[k : k + 1, :] = jnp.sum(jnp.where(hits[k], per_owner, 0.0), axis=0, keepdims=True).astype(BF)


def grad_pair_body(t_ref, x_ref, gg_ref, gu_ref, gate_ref, up_ref):
    t = t_ref[0]
    for j in range(SIDES):
        k = lax.rem(j - t + SIDES, SIDES)
        x = x_ref[pl.ds(k, 1)][0]
        for src, out in ((gg_ref, gate_ref), (gu_ref, up_ref)):
            out[:, WID * j : WID * j + WID] = dot(src[...], x, TN).astype(BF)[:, :WID]


def down_body(got, act_ref, act_tail_ref, out_ref, scaled):
    @pl.when(pl.program_id(0) == 0)
    def _():
        def store(row, lane, value):
            width = min(128, FEAT - lane)
            scaled[row : row + value.shape[0], lane : lane + width] = value[:, :width]

        unpack(got, FPAD, store)
        p_col = act_tail_ref[...].astype(F32)[:, PROB - 640 : PROB - 639]
        scaled[...] = (scaled[...].astype(F32) * p_col).astype(BF)

    out_ref[...] = dot(act_ref[...], scaled[...], TN).astype(BF)


def turn(w, t):
    return call(
        turn_body,
        struct((SIDES, WID, PAD)),
        grid=(3,),
        in_specs=[sm(), pl.BlockSpec((240, FEAT), lambda i: (i, 0))],
        out_specs=pl.BlockSpec((SIDES, 240, PAD), lambda i: (0, i, 0)),
        vmem=TURN_VMEM,
    )(t, w)


def hbm():
    return pl.BlockSpec(memory_space=pltpu.HBM)


def dma(*shape):
    return pltpu.SemaphoreType.DMA(shape)


def whole(shape):
    return pl.BlockSpec(shape, lambda i: (0,) * len(shape))


def hold(*values):
    return lax.optimization_barrier(values)


def shards(tokens, out_grad, route_probs, expert_ids, placement_map, w_gate, w_up, w_down):
    above = [((i + 1) % SIDES, i) for i in range(SIDES)]
    below = [((i - 1) % SIDES, i) for i in range(SIDES)]

    def from_above(value):
        return lax.ppermute(value, "tensor", above)

    def from_below(value):
        return lax.ppermute(value, "tensor", below)

    t = lax.axis_index("tensor").astype(jnp.int32).reshape(1)
    tok_t, d_t, ids_t, prob_t = tokens.T, out_grad.T, expert_ids.T, route_probs.T
    pmap = placement_map.reshape(1, -1)
    wg_t, wu_t, wd = w_gate[0].T, w_up[0].T, w_down[0]
    bx = block_rows(PAD)
    bd = block_rows(FPAD)
    t, d_t = hold(t, d_t)
    d_above, d_below = from_above(d_t), from_below(d_t)
    send_x, pick = call(
        dispatch_x_body,
        (struct((OWNERS, bx, 128)), struct((ROWS, TOK))),
        in_specs=[vm()] * 4,
        out_specs=(vm(), vm()),
        scratch_shapes=[pltpu.VMEM((PAD, TOK), BF), pltpu.VMEM((ROWS - MROWS, PAD), BF)],
        flops=10**9,
        vmem=60,
    )(ids_t, prob_t, pmap, tok_t)
    got_x = lax.all_to_all(send_x, "dp", 0, 0, tiled=True)
    d_far_a, d_far_b = from_below(d_below[:368]), from_above(d_above[368:])
    wg = turn(wg_t, t)
    wu = turn(wu_t, t)
    x_a, x_b = got_x[: OWNERS // 2], got_x[OWNERS // 2 :]
    x_below_a, x_above_b = from_below(x_a), from_above(x_b)
    x_below_b, x_above_a = from_below(x_b), from_above(x_a)
    send_d = call(
        dispatch_d_body,
        struct((OWNERS, bd, 128)),
        in_specs=[sm()] + [vm()] * 6,
        out_specs=vm(),
        scratch_shapes=[pltpu.VMEM((3072, TOK), BF), pltpu.VMEM((ROWS - MROWS, FPAD), BF)],
        flops=2 * 10**9,
        vmem=SEND_VMEM,
    )(t, pick, d_t, d_below, d_above, d_far_a, d_far_b)
    got_d = lax.all_to_all(send_d, "dp", 0, 0, tiled=True)
    x_far_a, x_far_b = from_below(x_below_a), from_above(x_above_b)
    act_spec = pl.BlockSpec((ROWS, 256), lambda i: (0, i))
    row_spec = pl.BlockSpec((256, FEAT), lambda i: (i, 0))
    mid = struct((ROWS, PAD))
    half, half32 = struct((HALF, PAD)), struct((HALF, PAD), F32)
    act, fgu, x_rel = call(
        gate_up_body,
        (struct((ROWS, PAD)), struct((2, ROWS, PAD)), struct((SIDES, ROWS, PAD))),
        in_specs=[hbm()] * 9,
        out_specs=(hbm(),) * 3,
        scratch_shapes=[
            pltpu.VMEM((SIDES, OWNERS, bx, 128), BF),
            pltpu.VMEM((2, SIDES, WID, PAD), BF),
            pltpu.VMEM((ROWS, PAD), BF),
            pltpu.VMEM((2, ROWS, PAD), BF),
            pltpu.VMEM((SIDES, ROWS, PAD), BF),
            dma(7),
            dma(6),
            dma(7),
        ],
        flops=5 * 10**9,
        vmem=GATE_VMEM,
    )(got_x, x_below_a, x_below_b, x_above_a, x_above_b, x_far_a, x_far_b, wg, wu)
    gg, gu, prob, part_a, part_b = call(
        back_body,
        (mid, mid, struct((ROWS, 128), F32), half, half),
        in_specs=[hbm()] * 6,
        out_specs=(hbm(),) * 2 + (vm(),) * 3,
        scratch_shapes=[
            pltpu.VMEM((OWNERS, bd, 128), BF),
            pltpu.VMEM((WID, FEAT), BF),
            pltpu.VMEM((ROWS, PAD), BF),
            pltpu.VMEM((2, ROWS, PAD), BF),
            pltpu.VMEM((ROWS, 2 * PAD), BF),
            pltpu.VMEM((2 * PAD, PAD), BF),
            pltpu.VMEM((ROWS, FEAT), BF),
            dma(4),
            dma(9),
            dma(2),
        ],
        flops=4 * 10**9,
        vmem=BACK_VMEM,
    )(got_d, wd, act, fgu, wg, wu)
    came_a, came_b = from_below(part_a), from_above(part_b)
    side = lambda k: pl.BlockSpec((1, WID, PAD), lambda i: (k, 0, 0))
    acts = [whole((ROWS, PAD))] * 2
    tail = [whole((ROWS, 128))]
    send_a, send_b, keep_a, keep_b = call(
        near_dx_body,
        (half, half, half32, half32),
        grid=(1,),
        in_specs=acts + [side(1), side(1), side(3), side(3)] + tail,
        out_specs=(whole((HALF, PAD)),) * 4,
        flops=24 * 10**8,
        vmem=NEAR_VMEM,
    )(gg, gu, wg, wu, wg, wu, prob)
    below_b, above_a = from_below(send_a), from_above(send_b)
    own = call(
        own_dx_body,
        struct((ROWS, PAD), F32),
        grid=(1,),
        in_specs=acts + [side(0), side(0)] + tail,
        out_specs=whole((ROWS, PAD)),
        flops=12 * 10**8,
        vmem=NEAR_VMEM,
    )(gg, gu, wg, wu, prob)
    pass_a, pass_b = call(relay_body, (half, half), in_specs=[vm()] * 4, out_specs=(vm(), vm()), vmem=10)(
        keep_a, came_a, keep_b, came_b
    )
    below_a, above_b = from_below(pass_a), from_above(pass_b)
    gate_grad, up_grad = call(
        grad_pair_body,
        (struct((WID, FEAT)), struct((WID, FEAT))),
        grid=(3,),
        in_specs=[sm(), whole((SIDES, ROWS, PAD)), act_spec, act_spec],
        out_specs=(row_spec, row_spec),
        flops=5 * 10**9,
        vmem=20,
    )(t, x_rel, gg, gu)
    below_a, above_b, gate_grad, up_grad = hold(below_a, above_b, gate_grad, up_grad)
    send_back = call(
        sum_body,
        struct((OWNERS, bx, 128)),
        in_specs=[vm()] * 5,
        out_specs=vm(),
        scratch_shapes=[pltpu.VMEM((ROWS - MROWS, PAD), BF)],
        vmem=10,
    )(own, below_a, below_b, above_a, above_b)
    back = lax.all_to_all(send_back, "dp", 0, 0, tiled=True)
    down_grad = call(
        down_body,
        struct((WID, FEAT)),
        grid=(3,),
        in_specs=[whole((OWNERS, bd, 128)), act_spec, pl.BlockSpec((ROWS, 128), lambda i: (0, 5))],
        out_specs=row_spec,
        scratch_shapes=[pltpu.VMEM((ROWS, FEAT), BF)],
        flops=3 * 10**9,
        vmem=20,
    )(got_d, act, act)
    dx_t, dp_t = call(
        combine_body,
        (struct((WID, TOK)), struct((TOP, TOK))),
        in_specs=[vm()] * 4,
        out_specs=(vm(), vm()),
        scratch_shapes=[pltpu.VMEM((ROWS, PAD), BF)],
        flops=10**9,
        vmem=10,
    )(back, pick, ids_t, pmap)
    return dx_t.T, gate_grad.T[None], up_grad.T[None], down_grad[None], dp_t.T


def solution(mesh):
    in_specs = (
        P("dp", "tensor"),
        P("dp", "tensor"),
        P("dp", None),
        P("dp", None),
        P(),
        P("dp", None, "tensor"),
        P("dp", None, "tensor"),
        P("dp", "tensor", None),
    )
    out_specs = (
        P("dp", "tensor"),
        P("dp", None, "tensor"),
        P("dp", None, "tensor"),
        P("dp", "tensor", None),
        P("dp", None),
    )

    return jax.shard_map(shards, mesh=mesh, in_specs=in_specs, out_specs=out_specs, check_vma=False)
```

```python
import jax
import jax.numpy as jnp
from jax import lax
from jax.experimental import pallas as pl
from jax.experimental.pallas import tpu as pltpu
from jax.sharding import PartitionSpec as P


SWISH_SLOPE = 1.702
EXP_OWN = 4
OWNERS = 32
CAP = 18
MAIN = 16
ROWS = OWNERS * CAP
MROWS = OWNERS * MAIN
TOK = 384
TOP = 4
WID = 720
PAD = 768
FEAT = 2880
FPAD = 2944
SIDES = 4
GATE_VMEM = 58
TURN_VMEM = 59
NEAR_VMEM = 20
SEND_VMEM = 44
BACK_VMEM = 52
PROB = 720

BF = jnp.bfloat16
F32 = jnp.float32
NT = (((1,), (1,)), ((), ()))
TN = (((0,), (0,)), ((), ()))
NN = (((1,), (0,)), ((), ()))


def dot(a, b, dims):
    return lax.dot_general(a, b, dims, preferred_element_type=F32)


def call(body, out_shape, **kw):
    params = pltpu.CompilerParams(vmem_limit_bytes=kw.pop("vmem", 8) << 20, **({"dimension_semantics": ("arbitrary",)} if "grid" in kw else {}))
    flops = kw.pop("flops", 0)
    nbytes = kw.pop("nbytes", 4 << 20)
    return pl.pallas_call(
        body,
        out_shape=out_shape,
        compiler_params=params,
        cost_estimate=pl.CostEstimate(flops=flops, bytes_accessed=nbytes, transcendentals=0),
        **kw,
    )


def struct(shape, dtype=BF):
    return jax.ShapeDtypeStruct(shape, dtype)


def vm():
    return pl.BlockSpec(memory_space=pltpu.VMEM)


def sm():
    return pl.BlockSpec(memory_space=pltpu.SMEM)


def iota(shape, dim):
    return lax.broadcasted_iota(jnp.int32, shape, dim)


def swap_matrix():
    r, q = iota((128, 128), 0), iota((128, 128), 1)
    return (((r >> 4) == ((q >> 1) & 7)) & ((q >> 4) == ((r >> 1) & 7)) & ((r & 1) == (q & 1))).astype(BF)


def tiles_of(width):
    return width // 128


def block_rows(width):
    t = tiles_of(width)
    return MAIN * t + 16 * ((t + 7) // 8)


def pack_rest(rest, out_ref, width):
    t = tiles_of(width)
    swap = swap_matrix()
    for a in range((t + 7) // 8):
        for i in range(OWNERS // 8):
            parts = [
                rest[16 * i : 16 * i + 16, 128 * j : 128 * j + 128] if j < t else jnp.zeros((16, 128), BF)
                for j in range(8 * a, 8 * a + 8)
            ]
            turned = dot(swap, jnp.concatenate(parts, axis=0), NN).astype(BF)
            out_ref[8 * i : 8 * i + 8, MAIN * t + 16 * a : MAIN * t + 16 * a + 16, :] = turned.reshape(8, 16, 128)


def unpack(ref, width, store, first=0):
    t = tiles_of(width)
    peers = ref.shape[0]
    for j in range(t):
        store(MAIN * first, 128 * j, ref[:, MAIN * j : MAIN * j + MAIN, :].reshape(MAIN * peers, 128))
    swap = swap_matrix()
    for a in range((t + 7) // 8):
        for i in range(peers // 8):
            block = ref[8 * i : 8 * i + 8, MAIN * t + 16 * a : MAIN * t + 16 * a + 16, :].reshape(128, 128)
            turned = dot(swap, block, NN).astype(BF)
            for b in range(8):
                j = 8 * a + b
                if j < t:
                    store(MROWS + 2 * first + 16 * i, 128 * j, turned[16 * b : 16 * b + 16])


def row_owner(shape, dim):
    r = iota(shape, dim)
    return jnp.where(r < MROWS, r >> 4, (r - MROWS) >> 1)


def row_slot(shape, dim):
    r = iota(shape, dim)
    return jnp.where(r < MROWS, r & 15, MAIN + (r & 1))


def hits_of(ids_ref, map_ref):
    experts = map_ref.shape[1]
    eq = map_ref[...] == EXP_OWN * iota((OWNERS, experts), 0)
    held = jnp.sum(jnp.where(eq, iota((OWNERS, experts), 1), 0), axis=1, keepdims=True)
    return [ids_ref[k : k + 1, :] == held for k in range(TOP)]


def dispatch_x_body(ids_ref, prob_ref, map_ref, tok_ref, send_ref, pick_ref, tokp, rest):
    hits = hits_of(ids_ref, map_ref)
    probs = prob_ref[...].astype(F32)
    named = hits[0] | hits[1] | hits[2] | hits[3]
    p_on = jnp.zeros((OWNERS, TOK), F32)
    for k in range(TOP):
        p_on = jnp.where(hits[k], probs[k : k + 1, :], p_on)
    upper = (iota((TOK, TOK), 0) < iota((TOK, TOK), 1)).astype(F32).astype(BF)
    rank = dot(named.astype(F32).astype(BF), upper, NN)
    key = jnp.where(named, rank, -1.0).astype(BF)
    spread = (row_owner((ROWS, OWNERS), 0) == iota((ROWS, OWNERS), 1)).astype(F32).astype(BF)
    pick = dot(spread, key, NN) == row_slot((ROWS, TOK), 0).astype(F32)
    p_col = jnp.sum(jnp.where(pick, dot(spread, p_on.astype(BF), NN), 0.0), axis=1, keepdims=True)
    pick = pick.astype(F32).astype(BF)
    pick_ref[...] = pick
    tokp[0:WID, :] = tok_ref[...]
    tokp[WID:PAD, :] = jnp.zeros((PAD - WID, TOK), BF)
    for q in range(3):
        val = dot(pick, tokp[256 * q : 256 * q + 256, :], NT)
        if q == 2:
            val = jnp.where(iota((ROWS, 256), 1) == PROB - 512, p_col, val)
        val = val.astype(BF)
        for j in (2 * q, 2 * q + 1):
            tile = val[:, 128 * (j - 2 * q) : 128 * (j - 2 * q) + 128]
            send_ref[:, MAIN * j : MAIN * j + MAIN, :] = tile[:MROWS].reshape(OWNERS, MAIN, 128)
            rest[:, 128 * j : 128 * j + 128] = tile[MROWS:]
    pack_rest(rest, send_ref, PAD)


def dispatch_d_body(t_ref, pick_ref, own_ref, below_ref, above_ref, far_a_ref, far_b_ref, send_ref, full, rest):
    t = t_ref[0]

    def put(side, ref, off, rows):
        j = lax.rem(t + side, SIDES)
        full[pl.ds(pl.multiple_of(WID * j + off, 16), rows), :] = ref[...]

    put(0, own_ref, 0, WID)
    put(3, below_ref, 0, WID)
    put(1, above_ref, 0, WID)
    put(2, far_a_ref, 0, 368)
    put(2, far_b_ref, 368, WID - 368)
    full[FEAT:3072, :] = jnp.zeros((3072 - FEAT, TOK), BF)
    pick = pick_ref[...]
    for q in range(12):
        val = dot(pick, full[256 * q : 256 * q + 256, :], NT).astype(BF)
        for j in (2 * q, 2 * q + 1):
            if j < tiles_of(FPAD):
                tile = val[:, 128 * (j - 2 * q) : 128 * (j - 2 * q) + 128]
                send_ref[:, MAIN * j : MAIN * j + MAIN, :] = tile[:MROWS].reshape(OWNERS, MAIN, 128)
                rest[:, 128 * j : 128 * j + 128] = tile[MROWS:]
    pack_rest(rest, send_ref, FPAD)


def turn_body(t_ref, w_ref, out_ref):
    t = t_ref[0]
    pieces = [w_ref[:, WID * j : WID * j + WID] for j in range(SIDES)]
    for k in range(SIDES):
        j = lax.rem(t + k, SIDES)
        piece = jnp.where(j == 0, pieces[0], jnp.where(j == 1, pieces[1], jnp.where(j == 2, pieces[2], pieces[3])))
        out_ref[k, :, 0:WID] = piece
        out_ref[k, :, WID:PAD] = jnp.zeros((piece.shape[0], PAD - WID), BF)


CHUNKS = ((0, 256), (256, 256), (512, WID - 512))


def copies(pairs, sems):
    out = []
    for n, (src, dst) in enumerate(pairs):
        copy = pltpu.make_async_copy(src, dst, sems.at[n])
        copy.start()
        out.append(copy)
    return out


def keep_side(x, side):
    def store(row, lane, value):
        x[side, row : row + value.shape[0], lane : lane + 128] = value

    return store


def gate_up_near_body(*refs):
    x_refs, w_refs, (part_out, x_out), (got, w, part, x, got_sems, in_sems, out_sems) = refs[:5], refs[5:7], refs[7:9], refs[9:]
    peers = [slice(0, OWNERS)] + [slice(0, OWNERS // 2), slice(OWNERS // 2, OWNERS)] * 2
    places = [0, 2, 2, 1, 1]
    blocks = [got.at[place, part_of] for place, part_of in zip(places, peers)]
    got_loads = copies(list(zip(x_refs, blocks)), got_sems)
    pairs = []
    for lo, size in CHUNKS:
        for n in range(2):
            pairs.append((w_refs[n].at[0:2, lo : lo + size, :], w.at[n, 0:2, lo : lo + size, :]))
            pairs.append((w_refs[n].at[3, lo : lo + size, :], w.at[n, 2, lo : lo + size, :]))
    loads = copies(pairs[:4], in_sems)
    for n, (place, part_of) in enumerate(zip(places, peers)):
        got_loads[n].wait()
        unpack(blocks[n], PAD, keep_side(x, place), part_of.start)
    loads += copies(pairs[4:], in_sems.at[4:])
    stores = copies([(x.at[0:2], x_out.at[0:2]), (x.at[2], x_out.at[3])], out_sems.at[3:])
    for c, (lo, size) in enumerate(CHUNKS):
        for copy in loads[4 * c : 4 * c + 4]:
            copy.wait()
        for n in range(2):
            part[n, :, lo : lo + size] = sum(dot(x[k], w[n, k, lo : lo + size, :], NT) for k in range(3))
        if c == 2:
            tile = x[0, :, 640:768].astype(F32)
            p_col = jnp.sum(jnp.where(iota((ROWS, 128), 1) == PROB - 640, tile, 0.0), axis=1, keepdims=True)
            part[0, :, WID:PAD] = jnp.broadcast_to(p_col, (ROWS, PAD - WID))
            part[1, :, WID:PAD] = jnp.zeros((ROWS, PAD - WID), F32)
        stores += copies([(part.at[:, :, lo : lo + 256], part_out.at[:, :, lo : lo + 256])], out_sems.at[c : c + 1])
    for copy in stores:
        copy.wait()


def gate_up_far_body(*refs):
    x_refs, part_hbm, w_refs, (act_out, mid_out, x_out), scratch = refs[:2], refs[2], refs[3:5], refs[6:9], refs[9:]
    got, w, part, act, mid, x, got_sems, in_sems, out_sems = scratch
    blocks = [got.at[0 : OWNERS // 2], got.at[OWNERS // 2 : OWNERS]]
    got_loads = copies(list(zip(x_refs, blocks)), got_sems)
    pairs = []
    for lo, size in CHUNKS:
        pairs += [(w_refs[n].at[2, lo : lo + size, :], w.at[n, lo : lo + size, :]) for n in range(2)]
        pairs.append((part_hbm.at[:, :, lo : lo + 256], part.at[:, :, lo : lo + 256]))
    loads = copies(pairs, in_sems)
    for n in range(2):
        got_loads[n].wait()
        unpack(blocks[n], PAD, keep_side(x, 0), n * OWNERS // 2)
    stores = copies([(x.at[0], x_out.at[2])], out_sems.at[6:])
    for c, (lo, size) in enumerate(CHUNKS):
        for copy in loads[3 * c : 3 * c + 3]:
            copy.wait()
        gate, up1 = (part[n, :, lo : lo + size] + dot(x[0], w[n, lo : lo + size, :], NT) for n in range(2))
        up1 = up1 + 1.0
        sig = 1.0 / (1.0 + jnp.exp(-SWISH_SLOPE * gate))
        glu = gate * sig
        act[:, lo : lo + size] = (glu * up1).astype(BF)
        mid[0, :, lo : lo + size] = (up1 * (sig + SWISH_SLOPE * glu * (1.0 - sig))).astype(BF)
        mid[1, :, lo : lo + size] = glu.astype(BF)
        if c == 2:
            act[:, WID:PAD] = part[0, :, WID:PAD].astype(BF)
            mid[:, :, WID:PAD] = jnp.zeros((2, ROWS, PAD - WID), BF)
        cols = slice(lo, lo + 256)
        stores += copies(
            [(act.at[:, cols], act_out.at[:, cols]), (mid.at[:, :, cols], mid_out.at[:, :, cols])], out_sems.at[2 * c : 2 * c + 2]
        )
    for copy in stores:
        copy.wait()


def back_body(
    got_hbm, wd_hbm, act_hbm, mid_hbm, wg_hbm, wu_hbm,
    gg_out, gu_out, prob_ref, a_ref, b_ref,
    got, wd, act, mid, g, w, d, got_sems, sems, out_sems,
):
    eights = [slice(8 * i, 8 * i + 8) for i in range(OWNERS // 8)]
    got_loads = copies([(got_hbm.at[part], got.at[part]) for part in eights], got_sems)
    pairs = []
    for lo, size in CHUNKS:
        cols = slice(lo, lo + 256)
        pairs += [
            (wd_hbm.at[lo : lo + size, :], wd.at[lo : lo + size, :]),
            (mid_hbm.at[:, :, cols], mid.at[:, :, cols]),
        ]
        if lo == 0:
            pairs.append((act_hbm, act))
    pairs += [(ref.at[2], w.at[PAD * n : PAD * n + WID, :]) for n, ref in enumerate((wg_hbm, wu_hbm))]
    loads = copies(pairs[:3], sems)

    def store(row, lane, value):
        width = min(128, FEAT - lane)
        d[row : row + value.shape[0], lane : lane + width] = value[:, :width]

    for part, copy in zip(eights, got_loads):
        copy.wait()
        unpack(got.at[part], FPAD, store, part.start)
    loads += copies(pairs[3:], sems.at[3:])
    for n in range(2):
        w[PAD * n + WID : PAD * n + PAD, :] = jnp.zeros((PAD - WID, PAD), BF)
        g[:, PAD * n + WID : PAD * n + PAD] = jnp.zeros((ROWS, PAD - WID), BF)
    total = jnp.zeros((ROWS, 1), F32)
    for c, (lo, size) in enumerate(CHUNKS):
        wait = loads[:3] if c == 0 else loads[2 * c + 1 : 2 * c + 3]
        wait[0].wait()
        down_back = dot(d[...], wd[lo : lo + size, :], NT)
        for copy in wait[1:]:
            copy.wait()
        if c == 0:
            p_col = act[:, 640:768].astype(F32)[:, PROB - 640 : PROB - 639]
        delta = p_col * down_back
        g[:, lo : lo + size] = (delta * mid[0, :, lo : lo + size]).astype(BF)
        g[:, PAD + lo : PAD + lo + size] = (delta * mid[1, :, lo : lo + size]).astype(BF)
        total = total + jnp.sum(act[:, lo : lo + size].astype(F32) * down_back, axis=1, keepdims=True)
    stores = copies([(g.at[:, 0:PAD], gg_out), (g.at[:, PAD : 2 * PAD], gu_out)], out_sems)
    prob = jnp.where(iota((ROWS, 128), 1) == PROB - 640, total, 0.0)
    prob_ref[...] = prob
    loads[7].wait()
    loads[8].wait()
    val = dot(g[...], w[...], NN)
    left, right = val[:, :640], split_prob(val[:, 640:768] + prob)
    put_rows(a_ref, left[:HALF], right[:HALF])
    put_rows(b_ref, left[HALF:], right[HALF:])
    for copy in stores:
        copy.wait()


def split_prob(tile):
    lane = iota(tile.shape, 1)
    total = jnp.sum(jnp.where(lane == PROB - 640, tile, 0.0), axis=1, keepdims=True)
    high = total.astype(BF).astype(F32)
    return jnp.where(lane == PROB - 640, high, jnp.where(lane == PROB - 639, total - high, tile))


def join_prob(tile):
    lane = iota(tile.shape, 1)
    total = jnp.sum(jnp.where((lane == PROB - 640) | (lane == PROB - 639), tile, 0.0), axis=1, keepdims=True)
    return jnp.where(lane == PROB - 640, total, jnp.where(lane == PROB - 639, 0.0, tile))


HALF = ROWS // 2


def dx_of(gg, gu, wg, wu, prob):
    val = dot(gg[:, :WID], wg, NN) + dot(gu[:, :WID], wu, NN)
    return val[:, :640], val[:, 640:768] + prob


def put_rows(ref, left, right):
    ref[:, 0:640] = left.astype(ref.dtype)
    ref[:, 640:768] = right.astype(ref.dtype)


def near_dx_body(gg_ref, gu_ref, wga_ref, wua_ref, wgb_ref, wub_ref, prob_ref, send_a, send_b, keep_a, keep_b):
    gg, gu, prob = gg_ref[...], gu_ref[...], prob_ref[...]
    left, right = dx_of(gg, gu, wga_ref[0], wua_ref[0], prob)
    put_rows(send_a, left[HALF:], split_prob(right)[HALF:])
    put_rows(keep_a, left[:HALF], right[:HALF])
    left, right = dx_of(gg, gu, wgb_ref[0], wub_ref[0], prob)
    put_rows(send_b, left[:HALF], split_prob(right)[:HALF])
    put_rows(keep_b, left[HALF:], right[HALF:])


def own_dx_body(gg_ref, gu_ref, wg_ref, wu_ref, prob_ref, out_ref):
    put_rows(out_ref, *dx_of(gg_ref[...], gu_ref[...], wg_ref[0], wu_ref[0], prob_ref[...]))


def relay_body(keep_a, came_a, keep_b, came_b, out_a, out_b):
    for keep, came, out in ((keep_a, came_a, out_a), (keep_b, came_b, out_b)):
        left = keep[:, 0:640] + came[:, 0:640].astype(F32)
        put_rows(out, left, split_prob(keep[:, 640:768] + join_prob(came[:, 640:768].astype(F32))))


def sum_body(own_ref, below_a, below_b, above_a, above_b, send_ref, rest):
    for j in range(tiles_of(PAD)):
        cols = slice(128 * j, 128 * j + 128)
        tile = [
            own_ref[lo : lo + HALF, cols] + below[:, cols].astype(F32) + above[:, cols].astype(F32)
            for lo, below, above in ((0, below_a, above_a), (HALF, below_b, above_b))
        ]
        tile = jnp.concatenate(tile, axis=0)
        if j == 5:
            tile = join_prob(tile)
        tile = tile.astype(BF)
        send_ref[:, MAIN * j : MAIN * j + MAIN, :] = tile[:MROWS].reshape(OWNERS, MAIN, 128)
        rest[:, cols] = tile[MROWS:]
    pack_rest(rest, send_ref, PAD)


def combine_body(back_ref, pick_ref, ids_ref, map_ref, dx_ref, dp_ref, rows):
    def store(row, lane, value):
        rows[row : row + value.shape[0], lane : lane + 128] = value

    unpack(back_ref, PAD, store)
    pick = pick_ref[...]
    dx_ref[...] = dot(rows[...], pick, TN)[:WID].astype(BF)
    tile = rows[:, 640:768].astype(F32)
    p_col = jnp.sum(jnp.where(iota((ROWS, 128), 1) == PROB - 640, tile, 0.0), axis=1, keepdims=True)
    spread = (row_owner((OWNERS, ROWS), 1) == iota((OWNERS, ROWS), 0)).astype(F32).astype(BF)
    per_owner = dot(spread, (pick.astype(F32) * p_col).astype(BF), NN)
    hits = hits_of(ids_ref, map_ref)
    for k in range(TOP):
        dp_ref[k : k + 1, :] = jnp.sum(jnp.where(hits[k], per_owner, 0.0), axis=0, keepdims=True).astype(BF)


def grad_pair_body(t_ref, x_ref, gg_ref, gu_ref, gate_ref, up_ref):
    t = t_ref[0]
    for j in range(SIDES):
        k = lax.rem(j - t + SIDES, SIDES)
        x = x_ref[pl.ds(k, 1)][0]
        for src, out in ((gg_ref, gate_ref), (gu_ref, up_ref)):
            out[:, WID * j : WID * j + WID] = dot(src[...], x, TN).astype(BF)[:, :WID]


def down_body(got, act_ref, act_tail_ref, out_ref, scaled):
    @pl.when(pl.program_id(0) == 0)
    def _():
        def store(row, lane, value):
            width = min(128, FEAT - lane)
            scaled[row : row + value.shape[0], lane : lane + width] = value[:, :width]

        unpack(got, FPAD, store)
        p_col = act_tail_ref[...].astype(F32)[:, PROB - 640 : PROB - 639]
        scaled[...] = (scaled[...].astype(F32) * p_col).astype(BF)

    out_ref[...] = dot(act_ref[...], scaled[...], TN).astype(BF)


def turn(w, t):
    return call(
        turn_body,
        struct((SIDES, WID, PAD)),
        grid=(3,),
        in_specs=[sm(), pl.BlockSpec((240, FEAT), lambda i: (i, 0))],
        out_specs=pl.BlockSpec((SIDES, 240, PAD), lambda i: (0, i, 0)),
        vmem=TURN_VMEM,
    )(t, w)


def hbm():
    return pl.BlockSpec(memory_space=pltpu.HBM)


def dma(*shape):
    return pltpu.SemaphoreType.DMA(shape)


def whole(shape):
    return pl.BlockSpec(shape, lambda i: (0,) * len(shape))


def hold(*values):
    return lax.optimization_barrier(values)


def shards(tokens, out_grad, route_probs, expert_ids, placement_map, w_gate, w_up, w_down):
    above = [((i + 1) % SIDES, i) for i in range(SIDES)]
    below = [((i - 1) % SIDES, i) for i in range(SIDES)]

    def from_above(value):
        return lax.ppermute(value, "tensor", above)

    def from_below(value):
        return lax.ppermute(value, "tensor", below)

    t = lax.axis_index("tensor").astype(jnp.int32).reshape(1)
    tok_t, d_t, ids_t, prob_t = tokens.T, out_grad.T, expert_ids.T, route_probs.T
    pmap = placement_map.reshape(1, -1)
    wg_t, wu_t, wd = w_gate[0].T, w_up[0].T, w_down[0]
    bx = block_rows(PAD)
    bd = block_rows(FPAD)
    t, d_t = hold(t, d_t)
    d_above, d_below = from_above(d_t), from_below(d_t)
    send_x, pick = call(
        dispatch_x_body,
        (struct((OWNERS, bx, 128)), struct((ROWS, TOK))),
        in_specs=[vm()] * 4,
        out_specs=(vm(), vm()),
        scratch_shapes=[pltpu.VMEM((PAD, TOK), BF), pltpu.VMEM((ROWS - MROWS, PAD), BF)],
        flops=10**9,
        vmem=60,
    )(ids_t, prob_t, pmap, tok_t)
    got_x = lax.all_to_all(send_x, "dp", 0, 0, tiled=True)
    d_far_a, d_far_b = from_below(d_below[:368]), from_above(d_above[368:])
    wg = turn(wg_t, t)
    wu = turn(wu_t, t)
    x_a, x_b = got_x[: OWNERS // 2], got_x[OWNERS // 2 :]
    x_below_a, x_above_b = from_below(x_a), from_above(x_b)
    x_below_b, x_above_a = from_below(x_b), from_above(x_a)
    send_d = call(
        dispatch_d_body,
        struct((OWNERS, bd, 128)),
        in_specs=[sm()] + [vm()] * 6,
        out_specs=vm(),
        scratch_shapes=[pltpu.VMEM((3072, TOK), BF), pltpu.VMEM((ROWS - MROWS, FPAD), BF)],
        flops=2 * 10**9,
        vmem=SEND_VMEM,
    )(t, pick, d_t, d_below, d_above, d_far_a, d_far_b)
    got_d = lax.all_to_all(send_d, "dp", 0, 0, tiled=True)
    x_far_a, x_far_b = from_below(x_below_a), from_above(x_above_b)
    act_spec = pl.BlockSpec((ROWS, 256), lambda i: (0, i))
    row_spec = pl.BlockSpec((256, FEAT), lambda i: (i, 0))
    mid = struct((ROWS, PAD))
    half, half32 = struct((HALF, PAD)), struct((HALF, PAD), F32)
    part, x_near = call(
        gate_up_near_body,
        (struct((2, ROWS, PAD), F32), struct((SIDES, ROWS, PAD))),
        in_specs=[hbm()] * 7,
        out_specs=(hbm(),) * 2,
        scratch_shapes=[
            pltpu.VMEM((3, OWNERS, bx, 128), BF),
            pltpu.VMEM((2, 3, WID, PAD), BF),
            pltpu.VMEM((2, ROWS, PAD), F32),
            pltpu.VMEM((3, ROWS, PAD), BF),
            dma(5),
            dma(12),
            dma(5),
        ],
        flops=4 * 10**9,
        vmem=GATE_VMEM,
    )(got_x, x_below_a, x_below_b, x_above_a, x_above_b, wg, wu)
    act, fgu, x_rel = call(
        gate_up_far_body,
        (struct((ROWS, PAD)), struct((2, ROWS, PAD)), struct((SIDES, ROWS, PAD))),
        in_specs=[hbm()] * 6,
        out_specs=(hbm(),) * 3,
        input_output_aliases={5: 2},
        scratch_shapes=[
            pltpu.VMEM((OWNERS, bx, 128), BF),
            pltpu.VMEM((2, WID, PAD), BF),
            pltpu.VMEM((2, ROWS, PAD), F32),
            pltpu.VMEM((ROWS, PAD), BF),
            pltpu.VMEM((2, ROWS, PAD), BF),
            pltpu.VMEM((1, ROWS, PAD), BF),
            dma(2),
            dma(9),
            dma(7),
        ],
        flops=15 * 10**8,
        vmem=GATE_VMEM,
    )(x_far_a, x_far_b, part, wg, wu, x_near)
    gg, gu, prob, part_a, part_b = call(
        back_body,
        (mid, mid, struct((ROWS, 128), F32), half, half),
        in_specs=[hbm()] * 6,
        out_specs=(hbm(),) * 2 + (vm(),) * 3,
        scratch_shapes=[
            pltpu.VMEM((OWNERS, bd, 128), BF),
            pltpu.VMEM((WID, FEAT), BF),
            pltpu.VMEM((ROWS, PAD), BF),
            pltpu.VMEM((2, ROWS, PAD), BF),
            pltpu.VMEM((ROWS, 2 * PAD), BF),
            pltpu.VMEM((2 * PAD, PAD), BF),
            pltpu.VMEM((ROWS, FEAT), BF),
            dma(4),
            dma(9),
            dma(2),
        ],
        flops=4 * 10**9,
        vmem=BACK_VMEM,
    )(got_d, wd, act, fgu, wg, wu)
    came_a, came_b = from_below(part_a), from_above(part_b)
    side = lambda k: pl.BlockSpec((1, WID, PAD), lambda i: (k, 0, 0))
    acts = [whole((ROWS, PAD))] * 2
    tail = [whole((ROWS, 128))]
    send_a, send_b, keep_a, keep_b = call(
        near_dx_body,
        (half, half, half32, half32),
        grid=(1,),
        in_specs=acts + [side(1), side(1), side(3), side(3)] + tail,
        out_specs=(whole((HALF, PAD)),) * 4,
        flops=24 * 10**8,
        vmem=NEAR_VMEM,
    )(gg, gu, wg, wu, wg, wu, prob)
    below_b, above_a = from_below(send_a), from_above(send_b)
    own = call(
        own_dx_body,
        struct((ROWS, PAD), F32),
        grid=(1,),
        in_specs=acts + [side(0), side(0)] + tail,
        out_specs=whole((ROWS, PAD)),
        flops=12 * 10**8,
        vmem=NEAR_VMEM,
    )(gg, gu, wg, wu, prob)
    pass_a, pass_b = call(relay_body, (half, half), in_specs=[vm()] * 4, out_specs=(vm(), vm()), vmem=10)(
        keep_a, came_a, keep_b, came_b
    )
    below_a, above_b = from_below(pass_a), from_above(pass_b)
    gate_grad, up_grad = call(
        grad_pair_body,
        (struct((WID, FEAT)), struct((WID, FEAT))),
        grid=(3,),
        in_specs=[sm(), whole((SIDES, ROWS, PAD)), act_spec, act_spec],
        out_specs=(row_spec, row_spec),
        flops=5 * 10**9,
        vmem=20,
    )(t, x_rel, gg, gu)
    below_a, above_b, gate_grad, up_grad = hold(below_a, above_b, gate_grad, up_grad)
    send_back = call(
        sum_body,
        struct((OWNERS, bx, 128)),
        in_specs=[vm()] * 5,
        out_specs=vm(),
        scratch_shapes=[pltpu.VMEM((ROWS - MROWS, PAD), BF)],
        vmem=10,
    )(own, below_a, below_b, above_a, above_b)
    back = lax.all_to_all(send_back, "dp", 0, 0, tiled=True)
    down_grad = call(
        down_body,
        struct((WID, FEAT)),
        grid=(3,),
        in_specs=[whole((OWNERS, bd, 128)), act_spec, pl.BlockSpec((ROWS, 128), lambda i: (0, 5))],
        out_specs=row_spec,
        scratch_shapes=[pltpu.VMEM((ROWS, FEAT), BF)],
        flops=3 * 10**9,
        vmem=20,
    )(got_d, act, act)
    dx_t, dp_t = call(
        combine_body,
        (struct((WID, TOK)), struct((TOP, TOK))),
        in_specs=[vm()] * 4,
        out_specs=(vm(), vm()),
        scratch_shapes=[pltpu.VMEM((ROWS, PAD), BF)],
        flops=10**9,
        vmem=10,
    )(back, pick, ids_t, pmap)
    return dx_t.T, gate_grad.T[None], up_grad.T[None], down_grad[None], dp_t.T


def solution(mesh):
    in_specs = (
        P("dp", "tensor"),
        P("dp", "tensor"),
        P("dp", None),
        P("dp", None),
        P(),
        P("dp", None, "tensor"),
        P("dp", None, "tensor"),
        P("dp", "tensor", None),
    )
    out_specs = (
        P("dp", "tensor"),
        P("dp", None, "tensor"),
        P("dp", None, "tensor"),
        P("dp", "tensor", None),
        P("dp", None),
    )

    return jax.shard_map(shards, mesh=mesh, in_specs=in_specs, out_specs=out_specs, check_vma=False)
```
